256 devices in a mesh: section: 16 (over y, z_hi, core), dp: 16 (over x, z_lo).
Axes of the slice: x: 4, y: 4, z: 8 (z_hi: 2, z_lo: 4; z = z_hi * 4 + z_lo), core: 2. Of those that a mesh axis runs over, the one named last changes fastest.
Arguments:
- student_states: bfloat16 [16, 2048, 2048], P('section', 'dp'), may hold values from -6 to 6
- teacher_states: bfloat16 [64, 2048, 7168], P('section', 'dp'), may hold values from -18 to 18
- projector: bfloat16 [16, 2048, 7168], P('section', None, 'dp'), may hold values from -0.125 to 0.125
- layer_map: int32 [16], replicated, may hold values from 0 to 60, as said below
- boundaries: int32 [17], replicated, may hold values from 0 to 61, as said below
- valid_counts: int32 [16], P('dp'), may hold values from 32 to 128, as said below
Outputs:
- student_grads: bfloat16 [16, 2048, 2048], P('section', 'dp')
- projector_grads: bfloat16 [16, 2048, 7168], P('section', None, 'dp')
- layer_losses: float32 [16], P('section')
The draws below stay inside these ranges and needn't reach their ends.
Inputs may be any that keep to these rules, and one draw needn't show every extreme that they name: Section k holds 4 or 3 teacher layers, three sections the smaller number; boundaries[0] is 0 and boundaries[16] is 61. Teacher layer layer_map[l] lies on a section from l - 2 to l + 2; student layers 0 and 15 pair with layers of sections 1 and 14, student layers 1 and 14 with layers of sections 3 and 12. `valid_counts`: the valid tokens stand first in their micro-batch; the last micro-batch is full.
All inputs are finite; a program needn't handle non-finite values.
Results may differ from the reference program's by a relative error of at most 0.015.
Values may be sent and summed in bfloat16 or wider, within the bound.
A program may use at most 128 MiB of HBM per device.

```python
import jax
import jax.numpy as jnp
from jax import lax

DS = 2048
DT = 7168
MB_TOK = 128
TL_DEV = 4
STUDENT_LAYERS = 16
SLOTS = 64
TOKENS = 2048
N_SECTION = 16
N_DP = 16


def section_plan(key):
    base = jax.random.fold_in(key, 17)
    first_key = jax.random.fold_in(base, 1)
    second_key = jax.random.fold_in(base, 2)
    third_key = jax.random.fold_in(base, 3)
    places = jnp.arange(N_SECTION, dtype=jnp.int32)
    shorter = (jax.random.permutation(first_key, N_SECTION) < 3).astype(jnp.int32)
    held = TL_DEV - shorter
    bounds = jnp.concatenate([jnp.zeros((1,), jnp.int32), jnp.cumsum(held).astype(jnp.int32)])
    offsets = jax.random.randint(second_key, (N_SECTION,), -2, 3).astype(jnp.int32)
    owners = jnp.clip(places + offsets, 0, N_SECTION - 1)
    owners = owners.at[1].set(3).at[N_SECTION - 2].set(N_SECTION - 4)
    owners = owners.at[0].set(1).at[N_SECTION - 1].set(N_SECTION - 2)
    within = jax.random.randint(third_key, (N_SECTION,), 0, TL_DEV).astype(jnp.int32) % held[owners]
    mapped = (bounds[owners] + within).astype(jnp.int32)
    return (bounds, mapped)


def draw_layer_map(key, part):
    return section_plan(key)[1]


def draw_boundaries(key, part):
    return section_plan(key)[0]


def draw_valid_counts(key, part):
    places = jnp.arange(N_DP, dtype=jnp.int32)
    lowest = MB_TOK // 4
    rising = lowest + (MB_TOK - lowest) * places // max(N_DP - 1, 1)
    jitter = jax.random.randint(jax.random.fold_in(key, 5), (N_DP,), 0, MB_TOK // 8 + 1).astype(jnp.int32)
    counts = jnp.clip(rising - jitter, lowest, MB_TOK).astype(jnp.int32)
    return counts.at[N_DP - 1].set(MB_TOK)


def levels(key, extent, pieces, least, largest):
    level = 1.0
    for position, shards_of in pieces:
        heights = jax.random.uniform(jax.random.fold_in(jax.random.fold_in(key, 6), position), (shards_of,), jnp.float32, least / len(pieces), largest / len(pieces))
        level = level * jnp.repeat(jnp.exp(heights), extent[position] // shards_of).reshape((-1,) + (1,) * (len(extent) - 1 - position))
    return level


def normal_values(stream_key, shape, scale, most, shards=(), kind=jnp.bfloat16):
    values = jax.random.normal(stream_key, shape, jnp.float32) * scale
    if len(shards) > 0:
        values = levels(stream_key, shape, shards, -0.22, 0.18) * values
    return jnp.clip(values, min=-most, max=most).astype(kind)


def setup_inputs(seed: int = 0) -> dict:
    streams_of = jax.random.split(jax.random.key(seed), 7)
    student_states = normal_values(streams_of[0], (STUDENT_LAYERS, TOKENS, DS), 1.0, 6.0, ((0, 16), (1, 16)))
    teacher_states = normal_values(streams_of[1], (SLOTS, TOKENS, DT), 3.0, 18.0, ((0, 16), (1, 16)))
    projector = normal_values(streams_of[2], (STUDENT_LAYERS, DS, DT), DS ** -0.5, 0.125, ((0, 16), (2, 16)))
    layer_map = draw_layer_map(jax.random.fold_in(streams_of[6], 71), 0)
    boundaries = draw_boundaries(jax.random.fold_in(streams_of[6], 71), 0)
    valid_counts = draw_valid_counts(jax.random.fold_in(streams_of[6], 71), 0)
    return dict(student_states=student_states, teacher_states=teacher_states, projector=projector, layer_map=layer_map, boundaries=boundaries, valid_counts=valid_counts)


loss_scale = 128.0
norm_eps = 1e-06

def reference(student_states, teacher_states, projector, layer_map, boundaries, valid_counts):
    rows = jnp.arange(TOKENS, dtype=jnp.int32)
    limit = valid_counts[rows // MB_TOK]
    valid = (rows % MB_TOK < limit).astype(jnp.float32)[:, None]
    total = jnp.sum(valid_counts).astype(jnp.float32)
    owners = lax.optimization_barrier(jnp.sum((boundaries[None, 1:N_SECTION] <= layer_map[:, None]).astype(jnp.int32), axis=1))
    slots = (owners * TL_DEV + layer_map - boundaries[owners]).astype(jnp.int32)
    group_width = DT // N_DP
    student_list = []
    projector_list = []
    loss_list = []
    for layer in range(STUDENT_LAYERS):
        wide = teacher_states[slots[layer]].astype(jnp.float32)
        target = (wide * lax.rsqrt(lax.optimization_barrier(jnp.mean(wide * wide, axis=1, keepdims=True)) + norm_eps)).astype(jnp.bfloat16)
        projected = jnp.dot(student_states[layer], projector[layer], preferred_element_type=jnp.float32)
        residual = projected - target.astype(jnp.float32)
        loss_list.append(jnp.sum(valid * residual * residual) / (total * DT))
        scaled = (valid * (loss_scale / total) * residual).astype(jnp.bfloat16)
        summed = jnp.zeros((TOKENS, DS), jnp.float32)
        for group in range(N_DP):
            left = scaled[:, group * group_width:(group + 1) * group_width]
            right = projector[layer][:, group * group_width:(group + 1) * group_width]
            piece = jnp.dot(left, right.T, preferred_element_type=jnp.float32).astype(jnp.bfloat16)
            summed = summed + piece.astype(jnp.float32)
        student_list.append(summed.astype(jnp.bfloat16))
        projector_list.append(jnp.dot(student_states[layer].T, scaled, preferred_element_type=jnp.float32).astype(jnp.bfloat16))
    return (jnp.stack(student_list), jnp.stack(projector_list), jnp.stack(loss_list))
```

```python
import functools

import jax
import jax.numpy as jnp
from jax import lax
from jax.experimental import pallas as pl
from jax.experimental.pallas import tpu as pltpu
from jax.sharding import Mesh
from jax.sharding import PartitionSpec as P

F32 = jnp.float32
BF16 = jnp.bfloat16
MESH = pl.DeviceIdType.MESH
loss_scale = 128.0
norm_eps = 1e-06
N = 4


def kernel(
    lm,
    bd,
    vc,
    x_hbm,
    t_hbm,
    w_hbm,
    gown,
    zrecv,
    pown,
    precv,
    loss,
    tv,
    blk,
    snd,
    rcv,
    yrcv,
    xall,
    wpair,
    tl,
    tc,
    sall,
    grads,
    xrecv,
    zsend,
    psend,
    cnt,
    lsum,
    sq,
    loc_sem,
    x_ss,
    x_rs,
    w_ss,
    w_rs,
    c_ss,
    c_rs,
    d_ss,
    d_rs,
    y_ss,
    y_rs,
    l_ss,
    l_rs,
    k_ss,
    k_rs,
    gx_ss,
    gx_rs,
    gz_ss,
    gz_rs,
    p_ss,
    p_rs,
    q_ss,
    q_rs,
):
    y, zh, c = lax.axis_index("y"), lax.axis_index("zh"), lax.axis_index("c")
    x, zl = lax.axis_index("x"), lax.axis_index("zl")
    here = y * 4 + zh * 2 + c
    me = x * N + zl
    xp = 3 - x
    half, pair = lax.rem(x, 2), lax.div(x, 2)
    wp = x + 1 - 2 * half
    y_to = lax.rem(y + 2 * zh - 1 + 4, 4)
    y_from = lax.rem(y - 2 * zh + 1 + 4, 4)
    tokens = x_hbm.shape[1]
    width = w_hbm.shape[2]
    rest = DT_GROUPS * width

    def z_at(k):
        return lax.rem(zl + k, N)

    def z_back(k):
        return lax.rem(zl + N - k, N)

    def send(src, dst, ss, rs, where):
        copy = pltpu.make_async_remote_copy(
            src_ref=src, dst_ref=dst, send_sem=ss, recv_sem=rs, device_id=where, device_id_type=MESH
        )
        copy.start()
        return copy

    def arrived(dst, ss, rs):
        pltpu.make_async_remote_copy(
            src_ref=dst,
            dst_ref=dst,
            send_sem=ss,
            recv_sem=rs,
            device_id={"c": 1 - c},
            device_id_type=MESH,
        ).wait_recv()

    sent = []
    t_copy = pltpu.make_async_copy(t_hbm, tv, loc_sem.at[0])
    t_copy.start()
    x_copy = pltpu.make_async_copy(x_hbm.at[0], xall.at[zl], loc_sem.at[1])
    x_copy.start()
    w_copy = pltpu.make_async_copy(w_hbm.at[0], wpair.at[half], loc_sem.at[2])
    w_copy.start()
    cnt[me] = jnp.full(cnt.shape[1:], vc[0], jnp.int32)

    others = [(kx, kz) for kx in range(N) for kz in range(N) if (kx, kz) != (0, 0)]
    barrier = pltpu.get_barrier_semaphore()
    greeted = [{"c": 1 - c}, {"y": y_to}, {"y": y_from}]
    greeted += [{"x": lax.rem(x + kx, N), "zl": z_at(kz)} for kx, kz in others]
    greeted += [{"zh": 1 - zh, "x": px, "zl": z_at(kz)} for px in (x, xp) for kz in range(N)]
    for where in greeted:
        pl.semaphore_signal(barrier, inc=1, device_id=where, device_id_type=MESH)
    pl.semaphore_wait(barrier, len(greeted))

    for k in (2, 1, 3):
        sent.append(
            send(x_hbm.at[0], xall.at[zl], x_ss.at[k], x_rs.at[zl], {"zl": z_at(k)})
        )
    sent.append(send(x_hbm.at[0], xall.at[N + zl], x_ss.at[0], x_rs.at[N + zl], {"x": xp}))
    sent.append(send(w_hbm.at[0], wpair.at[half], w_ss, w_rs, {"x": wp}))
    for n, (kx, kz) in enumerate(others):
        where = {"x": lax.rem(x + kx, N), "zl": z_at(kz)}
        sent.append(send(cnt.at[me], cnt.at[me], c_ss.at[n], c_rs.at[me], where))

    def plan(offset):
        to = here + offset
        inside = (to >= 0) & (to < 16)
        layer = lm[jnp.clip(to, 0, 15)]
        owner = jnp.int32(0)
        for k in range(1, 16):
            owner = owner + jnp.where(bd[k] <= layer, 1, 0)
        place = jnp.clip(layer - bd[here], 0, tv.shape[0] - 1)
        return place, jnp.where(inside & (owner == here), F32(1.0), F32(0.0))

    def normalize(offset, dst):
        place, keep = plan(offset)

        def rows16(r, carry):
            rows = pl.ds(pl.multiple_of(r * 16, 16), 16)
            h = tv[place, rows, :].astype(F32)
            scale = lax.rsqrt(jnp.mean(h * h, axis=1, keepdims=True) + norm_eps) * keep
            out = (h * scale).astype(BF16)
            for p in range(2):
                for z in range(N):
                    for e in range(2):
                        at = width * (8 * p + 4 * e + z)
                        dst[p * N + z, rows, e * width : (e + 1) * width] = out[:, at : at + width]
            return carry

        lax.fori_loop(0, tokens // 16, rows16, 0)

    def chunk(q, z):
        return (pair + q - 2 * pair * q) * N + z

    def merge(dst, other):
        def rows16(r, carry):
            rows = pl.ds(pl.multiple_of(r * 16, 16), 16)
            dst[rows, :] = dst[rows, :] + other[rows, :]
            return carry

        lax.fori_loop(0, tokens // 16, rows16, 0)

    t_copy.wait()
    for n, offset in enumerate((-1, 1)):
        normalize(offset, snd.at[n])
        sent.append(send(snd.at[n], rcv.at[n], d_ss.at[n], d_rs.at[n], {"c": 1 - c}))
    normalize(-2, blk.at[0])
    normalize(2, blk.at[2])
    arrived(rcv.at[1 - c], d_ss.at[1 - c], d_rs.at[1 - c])

    def merge_far(i, carry):
        merge(blk.at[2 * (1 - c), i], rcv.at[1 - c, i])
        return carry

    lax.fori_loop(0, 2 * N, merge_far, 0)
    order = [(q, k) for q in (1, 0) for k in (2, 1, 3, 0)]
    for q, k in order:
        i = chunk(q, z_at(k))
        sent.append(
            send(blk.at[2 * zh, i], yrcv.at[i], y_ss.at[i], y_rs.at[i], {"y": y_to})
        )
    normalize(0, blk.at[1])
    arrived(rcv.at[c], d_ss.at[c], d_rs.at[c])

    def merge_near(i, carry):
        merge(blk.at[1, i], rcv.at[c, i])
        return carry

    lax.fori_loop(0, 2 * N, merge_near, 0)
    for q, k in order:
        i = chunk(q, z_at(k))
        slot = q * N + zl
        if (q, k) == (0, 0):
            own = pltpu.make_async_copy(blk.at[1, i], tl.at[slot], loc_sem.at[3])
            own.start()
        else:
            where = {"x": xp, "zl": z_at(k)} if q else {"zl": z_at(k)}
            sent.append(send(blk.at[1, i], tl.at[slot], l_ss.at[q * N + k], l_rs.at[slot], where))

    for k in (2, 1, 3):
        z = z_back(k)
        arrived(xall.at[z], x_ss.at[k], x_rs.at[z])
        sent.append(send(xall.at[z], xall.at[N + z], x_ss.at[N + k], x_rs.at[N + z], {"x": xp}))

    for q, k in order:
        i = chunk(q, z_at(k))
        arrived(yrcv.at[i], y_ss.at[i], y_rs.at[i])
        merge(blk.at[2 * (1 - zh), i], yrcv.at[i])
        where = {"zh": 1 - zh, "x": xp if q else x, "zl": z_at(k)}
        sent.append(
            send(
                blk.at[2 * (1 - zh), i],
                tc.at[q * N + zl],
                k_ss.at[q * N + k],
                k_rs.at[q * N + zl],
                where,
            )
        )

    for n, (kx, kz) in enumerate(others):
        d = lax.rem(x + kx, N) * N + z_at(kz)
        arrived(cnt.at[d], c_ss.at[n], c_rs.at[d])
    total = cnt[0, 0:1, 0:1]
    for d in range(1, N * N):
        total = total + cnt[d, 0:1, 0:1]
    total = total.astype(F32)
    factor = loss_scale / total
    x_copy.wait()
    w_copy.wait()
    arrived(wpair.at[1 - half], w_ss, w_rs)
    own.wait()
    sq[...] = jnp.zeros_like(sq)

    def token_block(q, z):
        slot = q * N + z
        d = (xp if q else x) * N + z
        row = lax.broadcasted_iota(jnp.int32, (tokens, width), 0)
        valid = jnp.where(row < cnt[d, 0:1, 0:1], F32(1.0), F32(0.0))
        base = pl.multiple_of(slot * tokens, tokens)
        for e in range(2):
            at = slice(e * width, (e + 1) * width)
            target = tl[slot, :, at].astype(F32) + tc[slot, :, at].astype(F32)
            got = jnp.dot(xall[slot], wpair[e], preferred_element_type=F32)
            residual = got - target
            masked = valid * residual
            sq[...] += jnp.sum(masked * residual, axis=0, keepdims=True)
            sall[e, pl.ds(base, tokens), :] = (masked * factor).astype(BF16)
        nt = (((1,), (1,)), ((), ()))
        for m in range(4):
            cols = slice(m * 512, (m + 1) * 512)
            part = lax.dot_general(
                sall[0, pl.ds(base, tokens), :], wpair[0, cols, :], nt, preferred_element_type=F32
            )
            part += lax.dot_general(
                sall[1, pl.ds(base, tokens), :], wpair[1, cols, :], nt, preferred_element_type=F32
            )
            grads[slot, :, cols] = part.astype(BF16)

    def far_block(k, carry):
        z = lax.rem(zl + N - k, N)
        slot = N + z
        arrived(xall.at[slot], x_ss.at[k], x_rs.at[slot])
        arrived(tl.at[slot], l_ss.at[slot], l_rs.at[slot])
        arrived(tc.at[slot], k_ss.at[slot], k_rs.at[slot])
        token_block(1, z)
        send(grads.at[slot], xrecv.at[z], gx_ss.at[z], gx_rs.at[z], {"x": xp})
        return carry

    def near_block(k, carry):
        z = lax.rem(zl + N - k, N)

        @pl.when(k > 0)
        def _():
            arrived(tl.at[z], l_ss.at[z], l_rs.at[z])

        arrived(tc.at[z], k_ss.at[z], k_rs.at[z])
        token_block(0, z)
        return carry

    lax.fori_loop(0, N, far_block, 0)
    lax.fori_loop(0, N, near_block, 0)

    lsum[me] = jnp.full(lsum.shape[1:], jnp.sum(sq[...]), F32)
    for n, (kx, kz) in enumerate(others):
        where = {"x": lax.rem(x + kx, N), "zl": z_at(kz)}
        sent.append(send(lsum.at[me], lsum.at[me], q_ss.at[n], q_rs.at[me], where))

    students = 2048
    step = 256

    def project(e, dst):
        def columns(j, carry):
            cols = pl.ds(pl.multiple_of(j * step, step), step)
            total_part = jnp.zeros((step, width), F32)
            for b in range(2 * N):
                total_part += lax.dot_general(
                    xall[b, :, cols],
                    sall[e, b * tokens : (b + 1) * tokens, :],
                    (((0,), (0,)), ((), ())),
                    preferred_element_type=F32,
                )
            dst[cols, :] = total_part.astype(dst.dtype)
            return carry

        lax.fori_loop(0, students // step, columns, 0)

    project(1 - half, psend)
    sent.append(send(psend, precv, p_ss, p_rs, {"x": wp}))

    def summed(z, dst):
        def rows16(r, carry):
            rows = pl.ds(pl.multiple_of(r * 16, 16), 16)
            both = grads[z, rows, :].astype(F32) + xrecv[z, rows, :].astype(F32)
            dst[rows, :] = both.astype(dst.dtype)
            return carry

        arrived(xrecv.at[z], gx_ss.at[z], gx_rs.at[z])
        lax.fori_loop(0, tokens // 16, rows16, 0)

    for k in (1, 2, 3):
        z = z_back(k)
        summed(z, zsend.at[k - 1])
        sent.append(
            send(zsend.at[k - 1], zrecv.at[N - 1 - k], gz_ss.at[k - 1], gz_rs.at[N - 1 - k], {"zl": z})
        )
    project(half, pown)
    summed(zl, gown)

    for n, (kx, kz) in enumerate(others):
        d = lax.rem(x + kx, N) * N + z_at(kz)
        arrived(lsum.at[d], q_ss.at[n], q_rs.at[d])
    squares = lsum[0]
    for d in range(1, N * N):
        squares = squares + lsum[d]
    loss[...] = squares / (total * rest)

    for k in range(3):
        arrived(zrecv.at[k], gz_ss.at[k], gz_rs.at[k])
    arrived(precv, p_ss, p_rs)

    def far_sent(z, carry):
        pltpu.make_async_remote_copy(
            src_ref=grads.at[N + z],
            dst_ref=xrecv.at[z],
            send_sem=gx_ss.at[z],
            recv_sem=gx_rs.at[z],
            device_id={"x": xp},
            device_id_type=MESH,
        ).wait_send()
        return carry

    lax.fori_loop(0, N, far_sent, 0)
    for copy in sent:
        copy.wait_send()


DT_GROUPS = 16


def per_device(student_states, teacher_states, projector, layer_map, boundaries, valid_counts):
    slots, tokens, features = teacher_states.shape
    students = student_states.shape[2]
    width = projector.shape[2]
    any_space = pl.BlockSpec(memory_space=pl.ANY)
    smem = pl.BlockSpec(memory_space=pltpu.SMEM)
    vmem = pl.BlockSpec(memory_space=pltpu.VMEM)
    dma = pltpu.SemaphoreType.DMA
    piece = (2 * N, tokens, 2 * width)
    gown, zrecv, pown, precv, loss = pl.pallas_call(
        kernel,
        out_shape=(
            jax.ShapeDtypeStruct((tokens, students), F32),
            jax.ShapeDtypeStruct((3, tokens, students), BF16),
            jax.ShapeDtypeStruct((students, width), F32),
            jax.ShapeDtypeStruct((students, width), BF16),
            jax.ShapeDtypeStruct((8, 128), F32),
        ),
        in_specs=[smem, smem, smem, any_space, any_space, any_space],
        out_specs=(vmem, any_space, vmem, any_space, vmem),
        scratch_shapes=[
            pltpu.VMEM((slots, tokens, features), BF16),
            pltpu.VMEM((3, *piece), BF16),
            pltpu.VMEM((2, *piece), BF16),
            pltpu.VMEM((2, *piece), BF16),
            pltpu.VMEM(piece, BF16),
            pltpu.VMEM((2 * N, tokens, students), BF16),
            pltpu.VMEM((2, students, width), BF16),
            pltpu.VMEM(piece, BF16),
            pltpu.VMEM(piece, BF16),
            pltpu.VMEM((2, 2 * N * tokens, width), BF16),
            pltpu.VMEM((2 * N, tokens, students), BF16),
            pltpu.VMEM((N, tokens, students), BF16),
            pltpu.VMEM((3, tokens, students), BF16),
            pltpu.VMEM((students, width), BF16),
            pltpu.VMEM((N * N, 8, 128), jnp.int32),
            pltpu.VMEM((N * N, 8, 128), F32),
            pltpu.VMEM((1, width), F32),
            dma((4,)),
            dma((2 * N,)),
            dma((2 * N,)),
            dma,
            dma,
            dma((16,)),
            dma((16,)),
            dma((2,)),
            dma((2,)),
            dma((2 * N,)),
            dma((2 * N,)),
            dma((2 * N,)),
            dma((2 * N,)),
            dma((2 * N,)),
            dma((2 * N,)),
            dma((N,)),
            dma((N,)),
            dma((3,)),
            dma((3,)),
            dma,
            dma,
            dma((16,)),
            dma((16,)),
        ],
        compiler_params=pltpu.CompilerParams(
            collective_id=0, has_side_effects=True, vmem_limit_bytes=67043328
        ),
    )(layer_map, boundaries, valid_counts, student_states, teacher_states, projector)
    student_grad = gown
    for k in range(3):
        student_grad = student_grad + zrecv[k].astype(F32)
    projector_grad = pown + precv.astype(F32)
    return student_grad.astype(BF16)[None], projector_grad.astype(BF16)[None], loss[0, 0:1]


def solution(mesh):
    axes = ("y", "zh", "c", "x", "zl")
    split = Mesh(mesh.devices.reshape(4, 2, 2, N, N), axes)
    section, dp = axes[:3], axes[3:]
    return jax.shard_map(
        per_device,
        mesh=split,
        in_specs=(P(section, dp, None), P(section, dp, None), P(section, None, dp), P(), P(), P(dp)),
        out_specs=(P(section, dp, None), P(section, None, dp), P(section)),
        check_vma=False,
    )
```

```python
import functools

import jax
import jax.numpy as jnp
from jax import lax
from jax.experimental import pallas as pl
from jax.experimental.pallas import tpu as pltpu
from jax.sharding import Mesh
from jax.sharding import PartitionSpec as P

F32 = jnp.float32
BF16 = jnp.bfloat16
MESH = pl.DeviceIdType.MESH
loss_scale = 128.0
norm_eps = 1e-06
N = 4


def kernel(
    lm,
    bd,
    vc,
    x_hbm,
    t_hbm,
    w_hbm,
    gout,
    pown,
    precv,
    loss,
    tv,
    blk,
    snd,
    rcv,
    yrcv,
    xall,
    wpair,
    tl,
    tc,
    sall,
    grads,
    xrecv,
    zsend,
    zrecv,
    gown,
    psend,
    cnt,
    lsum,
    sq,
    loc_sem,
    xr_ss,
    xl_ss,
    xx_ss,
    x_rs,
    w_ss,
    w_rs,
    c_ss,
    c_rs,
    d_ss,
    d_rs,
    y_ss,
    y_rs,
    l_ss,
    l_rs,
    k_ss,
    k_rs,
    gx_ss,
    gx_rs,
    gz_ss,
    gz_rs,
    p_ss,
    p_rs,
    q_ss,
    q_rs,
):
    y, zh, c = lax.axis_index("y"), lax.axis_index("zh"), lax.axis_index("c")
    x, zl = lax.axis_index("x"), lax.axis_index("zl")
    here = y * 4 + zh * 2 + c
    me = x * N + zl
    xp = 3 - x
    half, pair = lax.rem(x, 2), lax.div(x, 2)
    wp = x + 1 - 2 * half
    y_to = lax.rem(y + 2 * zh - 1 + 4, 4)
    y_from = lax.rem(y - 2 * zh + 1 + 4, 4)
    tokens = x_hbm.shape[1]
    width = w_hbm.shape[1]
    students = w_hbm.shape[2]
    rest = DT_GROUPS * width

    def z_at(k):
        return lax.rem(zl + k, N)

    def z_back(k):
        return lax.rem(zl + N - k, N)

    def send(src, dst, ss, rs, where):
        copy = pltpu.make_async_remote_copy(
            src_ref=src, dst_ref=dst, send_sem=ss, recv_sem=rs, device_id=where, device_id_type=MESH
        )
        copy.start()
        return copy

    def arrived(dst, ss, rs):
        pltpu.make_async_remote_copy(
            src_ref=dst,
            dst_ref=dst,
            send_sem=ss,
            recv_sem=rs,
            device_id={"c": 1 - c},
            device_id_type=MESH,
        ).wait_recv()

    sent = []
    t_copy = pltpu.make_async_copy(t_hbm, tv, loc_sem.at[0])
    t_copy.start()
    x_copy = pltpu.make_async_copy(x_hbm.at[0], xall.at[zl], loc_sem.at[1])
    x_copy.start()
    w_copy = pltpu.make_async_copy(w_hbm.at[0], wpair.at[half], loc_sem.at[2])
    w_copy.start()
    cnt[me] = jnp.full(cnt.shape[1:], vc[0], jnp.int32)

    others = [(kx, kz) for kx in range(N) for kz in range(N) if (kx, kz) != (0, 0)]
    barrier = pltpu.get_barrier_semaphore()
    greeted = [{"c": 1 - c}, {"y": y_to}, {"y": y_from}]
    greeted += [{"x": lax.rem(x + kx, N), "zl": z_at(kz)} for kx, kz in others]
    greeted += [{"zh": 1 - zh, "x": px, "zl": z_at(kz)} for px in (x, xp) for kz in range(N)]
    for where in greeted:
        pl.semaphore_signal(barrier, inc=1, device_id=where, device_id_type=MESH)
    pl.semaphore_wait(barrier, len(greeted))

    def right(b, act):
        @pl.when(zl < N - 1)
        def _():
            act(x_block(b), xall.at[b], xr_ss.at[b], x_rs.at[b], {"zl": zl + 1})

    def left(b, act):
        @pl.when(zl > 0)
        def _():
            act(x_block(b), xall.at[b], xl_ss.at[b], x_rs.at[b], {"zl": zl - 1})

    def across(b, act):
        act(x_block(b), xall.at[N + b], xx_ss.at[b], x_rs.at[N + b], {"x": xp})

    def x_block(b):
        return x_hbm.at[0] if b is zl else xall.at[b]

    def from_left(j, act):
        @pl.when(zl - j >= 0)
        def _():
            right(zl - j, act)
            across(zl - j, act)

    def from_right(j, act):
        @pl.when(zl + j < N)
        def _():
            left(zl + j, act)
            across(zl + j, act)

    def forward(j):
        @pl.when(zl - j >= 0)
        def _():
            arrived(xall.at[zl - j], xx_ss.at[zl - j], x_rs.at[zl - j])

        from_left(j, send)

        @pl.when(zl + j < N)
        def _():
            arrived(xall.at[zl + j], xx_ss.at[zl + j], x_rs.at[zl + j])

        from_right(j, send)

    right(zl, send)
    left(zl, send)
    across(zl, send)
    sent.append(send(w_hbm.at[0], wpair.at[half], w_ss, w_rs, {"x": wp}))
    for n, (kx, kz) in enumerate(others):
        where = {"x": lax.rem(x + kx, N), "zl": z_at(kz)}
        sent.append(send(cnt.at[me], cnt.at[me], c_ss.at[n], c_rs.at[me], where))

    def plan(offset):
        to = here + offset
        inside = (to >= 0) & (to < 16)
        layer = lm[jnp.clip(to, 0, 15)]
        owner = jnp.int32(0)
        for k in range(1, 16):
            owner = owner + jnp.where(bd[k] <= layer, 1, 0)
        place = jnp.clip(layer - bd[here], 0, tv.shape[0] - 1)
        return place, jnp.where(inside & (owner == here), F32(1.0), F32(0.0))

    def normalize(offset, dst):
        place, keep = plan(offset)

        def rows16(r, carry):
            rows = pl.ds(pl.multiple_of(r * 16, 16), 16)
            h = tv[place, rows, :].astype(F32)
            scale = lax.rsqrt(jnp.mean(h * h, axis=1, keepdims=True) + norm_eps) * keep
            out = (h * scale).astype(BF16)
            for p in range(2):
                for z in range(N):
                    for e in range(2):
                        at = width * (8 * p + 4 * e + z)
                        dst[p * N + z, rows, e * width : (e + 1) * width] = out[:, at : at + width]
            return carry

        lax.fori_loop(0, tokens // 16, rows16, 0)

    def chunk(q, z):
        return (pair + q - 2 * pair * q) * N + z

    def merge(dst, other):
        def rows16(r, carry):
            rows = pl.ds(pl.multiple_of(r * 16, 16), 16)
            dst[rows, :] = dst[rows, :] + other[rows, :]
            return carry

        lax.fori_loop(0, tokens // 16, rows16, 0)

    t_copy.wait()
    for n, offset in enumerate((-1, 1)):
        normalize(offset, snd.at[n])
        sent.append(send(snd.at[n], rcv.at[n], d_ss.at[n], d_rs.at[n], {"c": 1 - c}))
    forward(1)
    normalize(-2, blk.at[0])
    normalize(2, blk.at[2])
    arrived(rcv.at[1 - c], d_ss.at[1 - c], d_rs.at[1 - c])

    def merge_far(i, carry):
        merge(blk.at[2 * (1 - c), i], rcv.at[1 - c, i])
        return carry

    lax.fori_loop(0, 2 * N, merge_far, 0)
    order = [(q, k) for q in (1, 0) for k in (1, 2, 3, 0)]
    for q, k in order:
        i = chunk(q, z_at(k))
        sent.append(
            send(blk.at[2 * zh, i], yrcv.at[i], y_ss.at[i], y_rs.at[i], {"y": y_to})
        )
    normalize(0, blk.at[1])
    arrived(rcv.at[c], d_ss.at[c], d_rs.at[c])

    def merge_near(i, carry):
        merge(blk.at[1, i], rcv.at[c, i])
        return carry

    lax.fori_loop(0, 2 * N, merge_near, 0)
    for q, k in order:
        i = chunk(q, z_at(k))
        slot = q * N + zl
        if (q, k) == (0, 0):
            own = pltpu.make_async_copy(blk.at[1, i], tl.at[slot], loc_sem.at[3])
            own.start()
        else:
            where = {"x": xp, "zl": z_at(k)} if q else {"zl": z_at(k)}
            sent.append(send(blk.at[1, i], tl.at[slot], l_ss.at[q * N + k], l_rs.at[slot], where))

    forward(2)

    for q, k in order:
        i = chunk(q, z_at(k))
        arrived(yrcv.at[i], y_ss.at[i], y_rs.at[i])
        merge(blk.at[2 * (1 - zh), i], yrcv.at[i])
        where = {"zh": 1 - zh, "x": xp if q else x, "zl": z_at(k)}
        sent.append(
            send(
                blk.at[2 * (1 - zh), i],
                tc.at[q * N + zl],
                k_ss.at[q * N + k],
                k_rs.at[q * N + zl],
                where,
            )
        )

    forward(3)

    for n, (kx, kz) in enumerate(others):
        d = lax.rem(x + kx, N) * N + z_at(kz)
        arrived(cnt.at[d], c_ss.at[n], c_rs.at[d])
    total = cnt[0, 0:1, 0:1]
    for d in range(1, N * N):
        total = total + cnt[d, 0:1, 0:1]
    total = total.astype(F32)
    factor = loss_scale / total
    x_copy.wait()
    w_copy.wait()
    arrived(wpair.at[1 - half], w_ss, w_rs)
    own.wait()
    sq[...] = jnp.zeros_like(sq)

    def token_block(q, z):
        slot = q * N + z
        d = (xp if q else x) * N + z
        row = lax.broadcasted_iota(jnp.int32, (tokens, width), 0)
        valid = jnp.where(row < cnt[d, 0:1, 0:1], F32(1.0), F32(0.0))
        base = pl.multiple_of(slot * tokens, tokens)
        nt = (((1,), (1,)), ((), ()))
        for e in range(2):
            at = slice(e * width, (e + 1) * width)
            target = tl[slot, :, at].astype(F32) + tc[slot, :, at].astype(F32)
            got = lax.dot_general(xall[slot], wpair[e], nt, preferred_element_type=F32)
            residual = got - target
            masked = valid * residual
            sq[...] += jnp.sum(masked * residual, axis=0, keepdims=True)
            sall[e, pl.ds(base, tokens), :] = (masked * factor).astype(BF16)
        for m in range(4):
            cols = slice(m * 512, (m + 1) * 512)
            part = jnp.dot(
                sall[0, pl.ds(base, tokens), :], wpair[0, :, cols], preferred_element_type=F32
            )
            part += jnp.dot(
                sall[1, pl.ds(base, tokens), :], wpair[1, :, cols], preferred_element_type=F32
            )
            grads[slot, :, cols] = part.astype(BF16)

    def far_block(k, carry):
        z = lax.rem(zl + N - k - 1, N)
        slot = N + z
        arrived(xall.at[slot], xx_ss.at[z], x_rs.at[slot])
        arrived(tl.at[slot], l_ss.at[slot], l_rs.at[slot])
        arrived(tc.at[slot], k_ss.at[slot], k_rs.at[slot])
        token_block(1, z)
        send(grads.at[slot], xrecv.at[z], gx_ss.at[z], gx_rs.at[z], {"x": xp})
        return carry

    def near_block(k, carry):
        z = lax.rem(zl + N - k - 1, N)

        @pl.when(k < N - 1)
        def _():
            arrived(tl.at[z], l_ss.at[z], l_rs.at[z])

        arrived(tc.at[z], k_ss.at[z], k_rs.at[z])
        token_block(0, z)
        return carry

    lax.fori_loop(0, N, far_block, 0)
    lax.fori_loop(0, N, near_block, 0)

    lsum[me] = jnp.full(lsum.shape[1:], jnp.sum(sq[...]), F32)
    for n, (kx, kz) in enumerate(others):
        where = {"x": lax.rem(x + kx, N), "zl": z_at(kz)}
        sent.append(send(lsum.at[me], lsum.at[me], q_ss.at[n], q_rs.at[me], where))

    step = 256

    def project(e, dst):
        def columns(j, carry):
            cols = pl.ds(pl.multiple_of(j * step, step), step)
            block = xall[:, :, cols].reshape(2 * N * tokens, step)
            total_part = lax.dot_general(
                sall[e], block, (((0,), (0,)), ((), ())), preferred_element_type=F32
            )
            dst[:, cols] = total_part.astype(dst.dtype)
            return carry

        lax.fori_loop(0, students // step, columns, 0)

    project(1 - half, psend)
    sent.append(send(psend, precv, p_ss, p_rs, {"x": wp}))

    def summed(z, dst):
        def rows16(r, carry):
            rows = pl.ds(pl.multiple_of(r * 16, 16), 16)
            both = grads[z, rows, :].astype(F32) + xrecv[z, rows, :].astype(F32)
            dst[rows, :] = both.astype(dst.dtype)
            return carry

        arrived(xrecv.at[z], gx_ss.at[z], gx_rs.at[z])
        lax.fori_loop(0, tokens // 16, rows16, 0)

    for k in (1, 2, 3):
        z = z_back(k)
        summed(z, zsend.at[k - 1])
        sent.append(
            send(zsend.at[k - 1], zrecv.at[N - 1 - k], gz_ss.at[k - 1], gz_rs.at[N - 1 - k], {"zl": z})
        )
    project(half, pown)
    summed(zl, gown)

    for n, (kx, kz) in enumerate(others):
        d = lax.rem(x + kx, N) * N + z_at(kz)
        arrived(lsum.at[d], q_ss.at[n], q_rs.at[d])
    squares = lsum[0]
    for d in range(1, N * N):
        squares = squares + lsum[d]
    loss[...] = squares / (total * rest)

    for k in range(3):
        arrived(zrecv.at[k], gz_ss.at[k], gz_rs.at[k])

    def result(r, carry):
        rows = pl.ds(pl.multiple_of(r * 16, 16), 16)
        value = gown[rows, :]
        for k in range(3):
            value = value + zrecv[k, rows, :].astype(F32)
        gout[rows, :] = value.astype(BF16)
        return carry

    lax.fori_loop(0, tokens // 16, result, 0)
    arrived(precv, p_ss, p_rs)

    def drain(src, dst, ss, rs, where):
        pltpu.make_async_remote_copy(
            src_ref=src, dst_ref=dst, send_sem=ss, recv_sem=rs, device_id=where, device_id_type=MESH
        ).wait_send()

    right(zl, drain)
    left(zl, drain)
    across(zl, drain)
    for j in (1, 2, 3):
        from_left(j, drain)
        from_right(j, drain)

    def far_sent(z, carry):
        drain(grads.at[N + z], xrecv.at[z], gx_ss.at[z], gx_rs.at[z], {"x": xp})
        return carry

    lax.fori_loop(0, N, far_sent, 0)
    for copy in sent:
        copy.wait_send()


DT_GROUPS = 16


def per_device(student_states, teacher_states, projector, layer_map, boundaries, valid_counts):
    slots, tokens, features = teacher_states.shape
    students = student_states.shape[2]
    weights = jnp.swapaxes(projector, 1, 2)
    width = weights.shape[1]
    any_space = pl.BlockSpec(memory_space=pl.ANY)
    smem = pl.BlockSpec(memory_space=pltpu.SMEM)
    vmem = pl.BlockSpec(memory_space=pltpu.VMEM)
    dma = pltpu.SemaphoreType.DMA
    piece = (2 * N, tokens, 2 * width)
    gout, pown, precv, loss = pl.pallas_call(
        kernel,
        out_shape=(
            jax.ShapeDtypeStruct((tokens, students), BF16),
            jax.ShapeDtypeStruct((width, students), F32),
            jax.ShapeDtypeStruct((width, students), BF16),
            jax.ShapeDtypeStruct((8, 128), F32),
        ),
        in_specs=[smem, smem, smem, any_space, any_space, any_space],
        out_specs=(vmem, vmem, any_space, vmem),
        scratch_shapes=[
            pltpu.VMEM((slots, tokens, features), BF16),
            pltpu.VMEM((3, *piece), BF16),
            pltpu.VMEM((2, *piece), BF16),
            pltpu.VMEM((2, *piece), BF16),
            pltpu.VMEM(piece, BF16),
            pltpu.VMEM((2 * N, tokens, students), BF16),
            pltpu.VMEM((2, width, students), BF16),
            pltpu.VMEM(piece, BF16),
            pltpu.VMEM(piece, BF16),
            pltpu.VMEM((2, 2 * N * tokens, width), BF16),
            pltpu.VMEM((2 * N, tokens, students), BF16),
            pltpu.VMEM((N, tokens, students), BF16),
            pltpu.VMEM((3, tokens, students), BF16),
            pltpu.VMEM((3, tokens, students), BF16),
            pltpu.VMEM((tokens, students), F32),
            pltpu.VMEM((width, students), BF16),
            pltpu.VMEM((N * N, 8, 128), jnp.int32),
            pltpu.VMEM((N * N, 8, 128), F32),
            pltpu.VMEM((1, width), F32),
            dma((4,)),
            dma((N,)),
            dma((N,)),
            dma((N,)),
            dma((2 * N,)),
            dma,
            dma,
            dma((16,)),
            dma((16,)),
            dma((2,)),
            dma((2,)),
            dma((2 * N,)),
            dma((2 * N,)),
            dma((2 * N,)),
            dma((2 * N,)),
            dma((2 * N,)),
            dma((2 * N,)),
            dma((N,)),
            dma((N,)),
            dma((3,)),
            dma((3,)),
            dma,
            dma,
            dma((16,)),
            dma((16,)),
        ],
        compiler_params=pltpu.CompilerParams(
            collective_id=0, has_side_effects=True, vmem_limit_bytes=67043328
        ),
    )(layer_map, boundaries, valid_counts, student_states, teacher_states, weights)
    projector_grad = (pown + precv.astype(F32)).astype(BF16)
    return gout[None], jnp.swapaxes(projector_grad, 0, 1)[None], loss[0, 0:1]


def solution(mesh):
    axes = ("y", "zh", "c", "x", "zl")
    split = Mesh(mesh.devices.reshape(4, 2, 2, N, N), axes)
    section, dp = axes[:3], axes[3:]
    return jax.shard_map(
        per_device,
        mesh=split,
        in_specs=(P(section, dp, None), P(section, dp, None), P(section, None, dp), P(), P(), P(dp)),
        out_specs=(P(section, dp, None), P(section, None, dp), P(section)),
        check_vma=False,
    )
```

```python
import functools

import jax
import jax.numpy as jnp
from jax import lax
from jax.experimental import pallas as pl
from jax.experimental.pallas import tpu as pltpu
from jax.sharding import Mesh
from jax.sharding import PartitionSpec as P

F32 = jnp.float32
BF16 = jnp.bfloat16
MESH = pl.DeviceIdType.MESH
loss_scale = 128.0
norm_eps = 1e-06
N = 4


def kernel(
    lm,
    bd,
    vc,
    x_hbm,
    t_hbm,
    w_hbm,
    gout,
    pout,
    loss,
    tv,
    blk,
    snd,
    rcv,
    yrcv,
    xall,
    wpair,
    tl,
    tc,
    sall,
    grads,
    xrecv,
    zsend,
    acc,
    psend,
    precv,
    pown,
    xex,
    sex,
    cnt,
    lsum,
    sq,
    loc_sem,
    xr_ss,
    xl_ss,
    xx_ss,
    x_rs,
    w_ss,
    w_rs,
    c_ss,
    c_rs,
    d_ss,
    d_rs,
    y_ss,
    y_rs,
    l_ss,
    l_rs,
    k_ss,
    k_rs,
    gx_ss,
    gx_rs,
    gz_ss,
    gz_rs,
    p_ss,
    p_rs,
    xe_ss,
    xe_rs,
    se_ss,
    se_rs,
    q_ss,
    q_rs,
):
    y, zh, c = lax.axis_index("y"), lax.axis_index("zh"), lax.axis_index("c")
    x, zl = lax.axis_index("x"), lax.axis_index("zl")
    here = y * 4 + zh * 2 + c
    me = x * N + zl
    xp = 3 - x
    half, pair = lax.rem(x, 2), lax.div(x, 2)
    wp = x + 1 - 2 * half
    y_to = lax.rem(y + 2 * zh - 1 + 4, 4)
    y_from = lax.rem(y - 2 * zh + 1 + 4, 4)
    tokens = x_hbm.shape[1]
    width = w_hbm.shape[1]
    students = w_hbm.shape[2]
    rest = DT_GROUPS * width

    def z_at(k):
        return lax.rem(zl + k, N)

    upper = zl >= N // 2
    inward = jnp.where(upper, N - 1 - zl, zl)

    def place(s):
        z = jnp.where(s == 0, 3, jnp.where(s == 1, 2, jnp.where(s == 2, 1 - inward, inward)))
        return jnp.where(upper, N - 1 - z, z)

    def send(src, dst, ss, rs, where):
        copy = pltpu.make_async_remote_copy(
            src_ref=src, dst_ref=dst, send_sem=ss, recv_sem=rs, device_id=where, device_id_type=MESH
        )
        copy.start()
        return copy

    def arrived(dst, ss, rs):
        pltpu.make_async_remote_copy(
            src_ref=dst,
            dst_ref=dst,
            send_sem=ss,
            recv_sem=rs,
            device_id={"c": 1 - c},
            device_id_type=MESH,
        ).wait_recv()

    sent = []
    t_copy = pltpu.make_async_copy(t_hbm, tv, loc_sem.at[0])
    t_copy.start()
    x_copy = pltpu.make_async_copy(x_hbm.at[0], xall.at[zl], loc_sem.at[1])
    x_copy.start()
    w_copy = pltpu.make_async_copy(w_hbm.at[0], wpair.at[half], loc_sem.at[2])
    w_copy.start()
    cnt[me] = jnp.full(cnt.shape[1:], vc[0], jnp.int32)

    others = [(kx, kz) for kx in range(N) for kz in range(N) if (kx, kz) != (0, 0)]
    barrier = pltpu.get_barrier_semaphore()
    greeted = [{"c": 1 - c}, {"y": y_to}, {"y": y_from}]
    greeted += [{"x": lax.rem(x + kx, N), "zl": z_at(kz)} for kx, kz in others]
    greeted += [{"zh": 1 - zh, "x": px, "zl": z_at(kz)} for px in (x, xp) for kz in range(N)]
    for where in greeted:
        pl.semaphore_signal(barrier, inc=1, device_id=where, device_id_type=MESH)
    pl.semaphore_wait(barrier, len(greeted))

    def right(b, act):
        @pl.when(zl < N - 1)
        def _():
            act(x_block(b), xall.at[b], xr_ss.at[b], x_rs.at[b], {"zl": zl + 1})

    def left(b, act):
        @pl.when(zl > 0)
        def _():
            act(x_block(b), xall.at[b], xl_ss.at[b], x_rs.at[b], {"zl": zl - 1})

    def across(b, act):
        act(x_block(b), xall.at[N + b], xx_ss.at[b], x_rs.at[N + b], {"x": xp})

    def x_block(b):
        return x_hbm.at[0] if b is zl else xall.at[b]

    def from_left(j, act):
        @pl.when(zl - j >= 0)
        def _():
            right(zl - j, act)
            across(zl - j, act)

    def from_right(j, act):
        @pl.when(zl + j < N)
        def _():
            left(zl + j, act)
            across(zl + j, act)

    def forward(j):
        @pl.when(zl - j >= 0)
        def _():
            arrived(xall.at[zl - j], xx_ss.at[zl - j], x_rs.at[zl - j])

        from_left(j, send)

        @pl.when(zl + j < N)
        def _():
            arrived(xall.at[zl + j], xx_ss.at[zl + j], x_rs.at[zl + j])

        from_right(j, send)

    right(zl, send)
    left(zl, send)
    across(zl, send)
    sent.append(send(w_hbm.at[0], wpair.at[half], w_ss, w_rs, {"x": wp}))
    for n, (kx, kz) in enumerate(others):
        where = {"x": lax.rem(x + kx, N), "zl": z_at(kz)}
        sent.append(send(cnt.at[me], cnt.at[me], c_ss.at[n], c_rs.at[me], where))

    def plan(offset):
        to = here + offset
        inside = (to >= 0) & (to < 16)
        layer = lm[jnp.clip(to, 0, 15)]
        owner = jnp.int32(0)
        for k in range(1, 16):
            owner = owner + jnp.where(bd[k] <= layer, 1, 0)
        slot = jnp.clip(layer - bd[here], 0, tv.shape[0] - 1)
        return slot, jnp.where(inside & (owner == here), F32(1.0), F32(0.0))

    def normalize(offset, dst):
        slot, keep = plan(offset)

        def rows16(r, carry):
            rows = pl.ds(pl.multiple_of(r * 16, 16), 16)
            h = tv[slot, rows, :].astype(F32)
            scale = lax.rsqrt(jnp.mean(h * h, axis=1, keepdims=True) + norm_eps) * keep
            out = (h * scale).astype(BF16)
            for p in range(2):
                for z in range(N):
                    for e in range(2):
                        at = width * (8 * p + 4 * e + z)
                        dst[p * N + z, rows, e * width : (e + 1) * width] = out[:, at : at + width]
            return carry

        lax.fori_loop(0, tokens // 16, rows16, 0)

    def chunk(q, z):
        return (pair + q - 2 * pair * q) * N + z

    def merge(dst, other):
        def rows16(r, carry):
            rows = pl.ds(pl.multiple_of(r * 16, 16), 16)
            dst[rows, :] = dst[rows, :] + other[rows, :]
            return carry

        lax.fori_loop(0, tokens // 16, rows16, 0)

    t_copy.wait()
    for n, offset in enumerate((-1, 1)):
        normalize(offset, snd.at[n])
        sent.append(send(snd.at[n], rcv.at[n], d_ss.at[n], d_rs.at[n], {"c": 1 - c}))
    forward(1)
    normalize(-2, blk.at[0])
    normalize(2, blk.at[2])
    arrived(rcv.at[1 - c], d_ss.at[1 - c], d_rs.at[1 - c])

    def merge_far(i, carry):
        merge(blk.at[2 * (1 - c), i], rcv.at[1 - c, i])
        return carry

    lax.fori_loop(0, 2 * N, merge_far, 0)
    order = [(q, s) for s in range(N) for q in (1, 0)]
    for q, s in order:
        i = chunk(q, place(s))
        sent.append(
            send(blk.at[2 * zh, i], yrcv.at[i], y_ss.at[i], y_rs.at[i], {"y": y_to})
        )
    normalize(0, blk.at[1])
    arrived(rcv.at[c], d_ss.at[c], d_rs.at[c])

    def merge_near(i, carry):
        merge(blk.at[1, i], rcv.at[c, i])
        return carry

    lax.fori_loop(0, 2 * N, merge_near, 0)
    def near(n):
        q, s = order[n]
        i = chunk(q, place(s))
        dst = tl.at[q * N + zl]
        if (q, s) == (0, N - 1):
            own = pltpu.make_async_copy(blk.at[1, i], dst, loc_sem.at[3])
            own.start()
            own.wait()
        else:
            where = {"x": xp if q else x, "zl": place(s)}
            sent.append(send(blk.at[1, i], dst, l_ss.at[q * N + s], l_rs.at[q * N + zl], where))

    near(0)
    near(1)
    for n, (q, s) in enumerate(order):
        i = chunk(q, place(s))
        slot = q * N + zl
        arrived(yrcv.at[i], y_ss.at[i], y_rs.at[i])
        merge(blk.at[2 * (1 - zh), i], yrcv.at[i])
        where = {"zh": 1 - zh, "x": xp if q else x, "zl": place(s)}
        sent.append(
            send(blk.at[2 * (1 - zh), i], tc.at[slot], k_ss.at[q * N + s], k_rs.at[slot], where)
        )
        if n + 2 < 2 * N:
            near(n + 2)
        if n == 1:
            forward(2)
        if n == 3:
            forward(3)

    for n, (kx, kz) in enumerate(others):
        d = lax.rem(x + kx, N) * N + z_at(kz)
        arrived(cnt.at[d], c_ss.at[n], c_rs.at[d])
    total = cnt[0, 0:1, 0:1]
    for d in range(1, N * N):
        total = total + cnt[d, 0:1, 0:1]
    total = total.astype(F32)
    factor = loss_scale / total
    x_copy.wait()
    w_copy.wait()
    arrived(wpair.at[1 - half], w_ss, w_rs)
    for z in range(N):
        arrived(xall.at[N + z], xx_ss.at[z], x_rs.at[N + z])
    for j in range(4):
        slot = (1 - j % 2) * N + place(2 + j // 2)
        sent.append(send(xall.at[slot], xex.at[j], xe_ss.at[j], xe_rs.at[j], {"x": wp}))
    sq[...] = jnp.zeros_like(sq)

    def token_block(q, z, n):
        slot = q * N + z
        d = jnp.where(q == 1, xp, x) * N + z
        row = lax.broadcasted_iota(jnp.int32, (tokens, width), 0)
        valid = jnp.where(row < cnt[d, 0:1, 0:1], F32(1.0), F32(0.0))
        base = pl.multiple_of(n * tokens, tokens)
        nt = (((1,), (1,)), ((), ()))
        for e in range(2):
            at = slice(e * width, (e + 1) * width)
            target = tl[slot, :, at].astype(F32) + tc[slot, :, at].astype(F32)
            got = lax.dot_general(xall[slot], wpair[e], nt, preferred_element_type=F32)
            residual = got - target
            masked = valid * residual
            sq[...] += jnp.sum(masked * residual, axis=0, keepdims=True)
            sall[e, pl.ds(base, tokens), :] = (masked * factor).astype(BF16)
        for m in range(4):
            cols = slice(m * 512, (m + 1) * 512)
            part = jnp.dot(
                sall[0, pl.ds(base, tokens), :], wpair[0, :, cols], preferred_element_type=F32
            )
            part += jnp.dot(
                sall[1, pl.ds(base, tokens), :], wpair[1, :, cols], preferred_element_type=F32
            )
            grads[slot, :, cols] = part.astype(BF16)

    step = 256

    def outer(e, terms, cols):
        value = None
        for t, mine in terms:
            if mine:
                left_rows = sall[e, 2 * t * tokens : (2 * t + 2) * tokens, :]
                blocks = [xall[N + place(t), :, cols], xall[place(t), :, cols]]
            else:
                left_rows = sex[2 * (t - 2) : 2 * (t - 1)].reshape(2 * tokens, width)
                blocks = [xex[2 * (t - 2), :, cols], xex[2 * (t - 2) + 1, :, cols]]
            part = lax.dot_general(
                left_rows,
                jnp.concatenate(blocks, axis=0),
                (((0,), (0,)), ((), ())),
                preferred_element_type=F32,
            )
            value = part if value is None else value + part
        return value

    def project(write):
        def columns(j, carry):
            write(pl.ds(pl.multiple_of(j * step, step), step))
            return carry

        lax.fori_loop(0, students // step, columns, 0)

    def to_partner(cols):
        psend[:, cols] = outer(1 - half, ((0, True), (1, True)), cols).astype(BF16)

    def first_steps(cols):
        terms = ((0, True), (1, True), (2, True), (2, False))
        pown[:, cols] = outer(half, terms, cols)

    def last_step(cols):
        value = pown[:, cols] + precv[:, cols].astype(F32)
        value = value + outer(half, ((3, True), (3, False)), cols)
        pout[:, cols] = value.astype(BF16)

    def extra_arrived(t):
        for j in (2 * (t - 2), 2 * (t - 2) + 1):
            arrived(xex.at[j], xe_ss.at[j], xe_rs.at[j])
            arrived(sex.at[j], se_ss.at[j], se_rs.at[j])

    def partner_piece(n):
        return sall.at[1 - half, pl.ds(pl.multiple_of(n * tokens, tokens), tokens)]

    def toward(s):
        return jnp.where(place(s) > zl, 0, 1)

    def add_rows(z, more, write):
        def rows16(r, carry):
            rows = pl.ds(pl.multiple_of(r * 16, 16), 16)
            both = grads[z, rows, :].astype(F32) + xrecv[z, rows, :].astype(F32)
            for way in more:
                both = both + acc[way, z, rows, :].astype(F32)
            write(rows, both.astype(BF16))
            return carry

        lax.fori_loop(0, tokens // 16, rows16, 0)

    def along(s, act):
        z, way = place(s), toward(s)
        act(
            zsend.at[s],
            acc.at[way, z],
            gz_ss.at[s],
            gz_rs.at[way * N + z],
            {"zl": zl + 1 - 2 * way},
        )

    def pass_on(s):
        z, way = place(s), toward(s)
        joined = jnp.where(way == 0, zl > 0, zl < N - 1)

        def put(rows, value):
            zsend[s, rows, :] = value

        arrived(xrecv.at[z], gx_ss.at[z], gx_rs.at[z])

        @pl.when(joined)
        def _():
            arrived(acc.at[way, z], gz_ss.at[s], gz_rs.at[way * N + z])
            add_rows(z, (way,), put)

        @pl.when(jnp.logical_not(joined))
        def _():
            add_rows(z, (), put)

        along(s, send)

    def one_block(n, carry):
        s, q = lax.div(n, 2), 1 - lax.rem(n, 2)
        z = place(s)
        slot = q * N + z

        @pl.when((q == 1) & (s > 0))
        def _():
            pass_on(s - 1)

        @pl.when(n == 4)
        def _():
            project(to_partner)
            send(psend, precv, p_ss, p_rs, {"x": wp})

        @pl.when(n == 6)
        def _():
            extra_arrived(2)
            project(first_steps)

        @pl.when(n < 2 * N - 1)
        def _():
            arrived(tl.at[slot], l_ss.at[slot], l_rs.at[slot])

        arrived(tc.at[slot], k_ss.at[slot], k_rs.at[slot])
        token_block(q, z, n)

        @pl.when(q == 1)
        def _():
            send(grads.at[slot], xrecv.at[z], gx_ss.at[z], gx_rs.at[z], {"x": xp})

        @pl.when(n >= 4)
        def _():
            send(partner_piece(n), sex.at[n - 4], se_ss.at[n - 4], se_rs.at[n - 4], {"x": wp})

        return carry

    lax.fori_loop(0, 2 * N, one_block, 0)

    lsum[me] = jnp.full(lsum.shape[1:], jnp.sum(sq[...]), F32)
    for n, (kx, kz) in enumerate(others):
        where = {"x": lax.rem(x + kx, N), "zl": z_at(kz)}
        sent.append(send(lsum.at[me], lsum.at[me], q_ss.at[n], q_rs.at[me], where))

    arrived(precv, p_ss, p_rs)
    extra_arrived(3)
    project(last_step)

    def put_out(rows, value):
        gout[rows, :] = value

    arrived(xrecv.at[zl], gx_ss.at[zl], gx_rs.at[zl])

    @pl.when(zl > 0)
    def _():
        arrived(acc.at[0, zl], gz_ss.at[0], gz_rs.at[zl])

    @pl.when(zl < N - 1)
    def _():
        arrived(acc.at[1, zl], gz_ss.at[0], gz_rs.at[N + zl])

    for low, high, ways in ((0, 1, (1,)), (1, N - 1, (0, 1)), (N - 1, N, (0,))):

        @pl.when((zl >= low) & (zl < high))
        def _():
            add_rows(zl, ways, put_out)

    for n, (kx, kz) in enumerate(others):
        d = lax.rem(x + kx, N) * N + z_at(kz)
        arrived(lsum.at[d], q_ss.at[n], q_rs.at[d])
    squares = lsum[0]
    for d in range(1, N * N):
        squares = squares + lsum[d]
    loss[0] = jnp.max(squares / (total * rest))

    def drain(src, dst, ss, rs, where):
        pltpu.make_async_remote_copy(
            src_ref=src, dst_ref=dst, send_sem=ss, recv_sem=rs, device_id=where, device_id_type=MESH
        ).wait_send()

    right(zl, drain)
    left(zl, drain)
    across(zl, drain)
    for j in (1, 2, 3):
        from_left(j, drain)
        from_right(j, drain)

    def far_sent(z, carry):
        drain(grads.at[N + z], xrecv.at[z], gx_ss.at[z], gx_rs.at[z], {"x": xp})
        return carry

    lax.fori_loop(0, N, far_sent, 0)
    drain(psend, precv, p_ss, p_rs, {"x": wp})
    for s in range(3):
        along(s, drain)
    for n in range(4, 2 * N):
        drain(partner_piece(n), sex.at[n - 4], se_ss.at[n - 4], se_rs.at[n - 4], {"x": wp})
    for copy in sent:
        copy.wait_send()


DT_GROUPS = 16


def per_device(student_states, teacher_states, projector, layer_map, boundaries, valid_counts):
    slots, tokens, features = teacher_states.shape
    students = student_states.shape[2]
    weights = jnp.swapaxes(projector, 1, 2)
    width = weights.shape[1]
    any_space = pl.BlockSpec(memory_space=pl.ANY)
    smem = pl.BlockSpec(memory_space=pltpu.SMEM)
    vmem = pl.BlockSpec(memory_space=pltpu.VMEM)
    dma = pltpu.SemaphoreType.DMA
    piece = (2 * N, tokens, 2 * width)
    gout, pout, loss = pl.pallas_call(
        kernel,
        out_shape=(
            jax.ShapeDtypeStruct((tokens, students), BF16),
            jax.ShapeDtypeStruct((width, students), BF16),
            jax.ShapeDtypeStruct((1,), F32),
        ),
        in_specs=[smem, smem, smem, any_space, any_space, any_space],
        out_specs=(vmem, vmem, smem),
        scratch_shapes=[
            pltpu.VMEM((slots, tokens, features), BF16),
            pltpu.VMEM((3, *piece), BF16),
            pltpu.VMEM((2, *piece), BF16),
            pltpu.VMEM((2, *piece), BF16),
            pltpu.VMEM(piece, BF16),
            pltpu.VMEM((2 * N, tokens, students), BF16),
            pltpu.VMEM((2, width, students), BF16),
            pltpu.VMEM(piece, BF16),
            pltpu.VMEM(piece, BF16),
            pltpu.VMEM((2, 2 * N * tokens, width), BF16),
            pltpu.VMEM((2 * N, tokens, students), BF16),
            pltpu.VMEM((N, tokens, students), BF16),
            pltpu.VMEM((3, tokens, students), BF16),
            pltpu.VMEM((2, N, tokens, students), BF16),
            pltpu.VMEM((width, students), BF16),
            pltpu.VMEM((width, students), BF16),
            pltpu.VMEM((width, students), F32),
            pltpu.VMEM((4, tokens, students), BF16),
            pltpu.VMEM((4, tokens, width), BF16),
            pltpu.VMEM((N * N, 8, 128), jnp.int32),
            pltpu.VMEM((N * N, 8, 128), F32),
            pltpu.VMEM((1, width), F32),
            dma((4,)),
            dma((N,)),
            dma((N,)),
            dma((N,)),
            dma((2 * N,)),
            dma,
            dma,
            dma((16,)),
            dma((16,)),
            dma((2,)),
            dma((2,)),
            dma((2 * N,)),
            dma((2 * N,)),
            dma((2 * N,)),
            dma((2 * N,)),
            dma((2 * N,)),
            dma((2 * N,)),
            dma((N,)),
            dma((N,)),
            dma((3,)),
            dma((2 * N,)),
            dma,
            dma,
            dma((4,)),
            dma((4,)),
            dma((4,)),
            dma((4,)),
            dma((16,)),
            dma((16,)),
        ],
        compiler_params=pltpu.CompilerParams(
            collective_id=0, has_side_effects=True, vmem_limit_bytes=67043328
        ),
    )(layer_map, boundaries, valid_counts, student_states, teacher_states, weights)
    return gout[None], jnp.swapaxes(pout, 0, 1)[None], loss


def solution(mesh):
    axes = ("y", "zh", "c", "x", "zl")
    split = Mesh(mesh.devices.reshape(4, 2, 2, N, N), axes)
    section, dp = axes[:3], axes[3:]
    return jax.shard_map(
        per_device,
        mesh=split,
        in_specs=(P(section, dp, None), P(section, dp, None), P(section, None, dp), P(), P(), P(dp)),
        out_specs=(P(section, dp, None), P(section, None, dp), P(section)),
        check_vma=False,
    )
```

```python
import functools

import jax
import jax.numpy as jnp
from jax import lax
from jax.experimental import pallas as pl
from jax.experimental.pallas import tpu as pltpu
from jax.sharding import Mesh
from jax.sharding import PartitionSpec as P

F32 = jnp.float32
BF16 = jnp.bfloat16
MESH = pl.DeviceIdType.MESH
loss_scale = 128.0
norm_eps = 1e-06
N = 4


def kernel(
    lm,
    bd,
    vc,
    x_hbm,
    t_hbm,
    w_hbm,
    gout,
    pout,
    loss,
    tv,
    blk,
    snd,
    rcv,
    yrcv,
    xall,
    wpair,
    tl,
    tc,
    sall,
    grads,
    xrecv,
    zsend,
    acc,
    psend,
    precv,
    pown,
    xex,
    sex,
    cnt,
    lsum,
    sq,
    loc_sem,
    xr_ss,
    xl_ss,
    xx_ss,
    x_rs,
    w_ss,
    w_rs,
    c_ss,
    c_rs,
    d_ss,
    d_rs,
    y_ss,
    y_rs,
    l_ss,
    l_rs,
    k_ss,
    k_rs,
    gx_ss,
    gx_rs,
    gz_ss,
    gz_rs,
    p_ss,
    p_rs,
    xe_ss,
    xe_rs,
    se_ss,
    se_rs,
    q_ss,
    q_rs,
):
    y, zh, c = lax.axis_index("y"), lax.axis_index("zh"), lax.axis_index("c")
    x, zl = lax.axis_index("x"), lax.axis_index("zl")
    here = y * 4 + zh * 2 + c
    me = x * N + zl
    xp = 3 - x
    half, pair = lax.rem(x, 2), lax.div(x, 2)
    wp = x + 1 - 2 * half
    y_to = lax.rem(y + 2 * zh - 1 + 4, 4)
    y_from = lax.rem(y - 2 * zh + 1 + 4, 4)
    tokens = x_hbm.shape[1]
    width = w_hbm.shape[1]
    students = w_hbm.shape[2]
    rest = DT_GROUPS * width

    def z_at(k):
        return lax.rem(zl + k, N)

    upper = zl >= N // 2
    inward = jnp.where(upper, N - 1 - zl, zl)

    def place(s):
        z = jnp.where(s == 0, 3, jnp.where(s == 1, 2, jnp.where(s == 2, 1 - inward, inward)))
        return jnp.where(upper, N - 1 - z, z)

    def send(src, dst, ss, rs, where):
        copy = pltpu.make_async_remote_copy(
            src_ref=src, dst_ref=dst, send_sem=ss, recv_sem=rs, device_id=where, device_id_type=MESH
        )
        copy.start()
        return copy

    def arrived(dst, ss, rs):
        pltpu.make_async_remote_copy(
            src_ref=dst,
            dst_ref=dst,
            send_sem=ss,
            recv_sem=rs,
            device_id={"c": 1 - c},
            device_id_type=MESH,
        ).wait_recv()

    sent = []
    t_copy = pltpu.make_async_copy(t_hbm, tv, loc_sem.at[0])
    t_copy.start()
    x_copy = pltpu.make_async_copy(x_hbm.at[0], xall.at[zl], loc_sem.at[1])
    x_copy.start()
    w_copy = pltpu.make_async_copy(w_hbm.at[0], wpair.at[half], loc_sem.at[2])
    w_copy.start()
    cnt[me] = jnp.full(cnt.shape[1:], vc[0], jnp.int32)

    others = [(kx, kz) for kx in range(N) for kz in range(N) if (kx, kz) != (0, 0)]
    barrier = pltpu.get_barrier_semaphore()
    greeted = [{"c": 1 - c}, {"y": y_to}, {"y": y_from}]
    greeted += [{"x": lax.rem(x + kx, N), "zl": z_at(kz)} for kx, kz in others]
    greeted += [{"zh": 1 - zh, "x": px, "zl": z_at(kz)} for px in (x, xp) for kz in range(N)]
    for where in greeted:
        pl.semaphore_signal(barrier, inc=1, device_id=where, device_id_type=MESH)
    pl.semaphore_wait(barrier, len(greeted))

    def right(b, act):
        @pl.when(zl < N - 1)
        def _():
            act(x_block(b), xall.at[b], xr_ss.at[b], x_rs.at[b], {"zl": zl + 1})

    def left(b, act):
        @pl.when(zl > 0)
        def _():
            act(x_block(b), xall.at[b], xl_ss.at[b], x_rs.at[b], {"zl": zl - 1})

    def across(b, act):
        act(x_block(b), xall.at[N + b], xx_ss.at[b], x_rs.at[N + b], {"x": xp})

    def x_block(b):
        return x_hbm.at[0] if b is zl else xall.at[b]

    def from_left(j, act):
        @pl.when(zl - j >= 0)
        def _():
            right(zl - j, act)
            across(zl - j, act)

    def from_right(j, act):
        @pl.when(zl + j < N)
        def _():
            left(zl + j, act)
            across(zl + j, act)

    def forward(j):
        @pl.when(zl - j >= 0)
        def _():
            arrived(xall.at[zl - j], xx_ss.at[zl - j], x_rs.at[zl - j])

        from_left(j, send)

        @pl.when(zl + j < N)
        def _():
            arrived(xall.at[zl + j], xx_ss.at[zl + j], x_rs.at[zl + j])

        from_right(j, send)

    def extra(j):
        slot = (1 - j % 2) * N + place(2 + j // 2)
        block = x_hbm.at[0] if j == 3 else xall.at[slot]
        sent.append(send(block, xex.at[j], xe_ss.at[j], xe_rs.at[j], {"x": wp}))

    right(zl, send)
    left(zl, send)
    across(zl, send)
    sent.append(send(w_hbm.at[0], wpair.at[half], w_ss, w_rs, {"x": wp}))
    for n, (kx, kz) in enumerate(others):
        where = {"x": lax.rem(x + kx, N), "zl": z_at(kz)}
        sent.append(send(cnt.at[me], cnt.at[me], c_ss.at[n], c_rs.at[me], where))

    def plan(offset):
        to = here + offset
        inside = (to >= 0) & (to < 16)
        layer = lm[jnp.clip(to, 0, 15)]
        owner = jnp.int32(0)
        for k in range(1, 16):
            owner = owner + jnp.where(bd[k] <= layer, 1, 0)
        slot = jnp.clip(layer - bd[here], 0, tv.shape[0] - 1)
        return slot, jnp.where(inside & (owner == here), F32(1.0), F32(0.0))

    def normalize(offset, dst):
        slot, keep = plan(offset)

        def rows16(r, carry):
            rows = pl.ds(pl.multiple_of(r * 16, 16), 16)
            h = tv[slot, rows, :].astype(F32)
            scale = lax.rsqrt(jnp.mean(h * h, axis=1, keepdims=True) + norm_eps) * keep
            out = (h * scale).astype(BF16)
            for p in range(2):
                for z in range(N):
                    for e in range(2):
                        at = width * (8 * p + 4 * e + z)
                        dst[p * N + z, rows, e * width : (e + 1) * width] = out[:, at : at + width]
            return carry

        lax.fori_loop(0, tokens // 16, rows16, 0)

    def chunk(q, z):
        return (pair + q - 2 * pair * q) * N + z

    def merge(dst, other):
        def rows16(r, carry):
            rows = pl.ds(pl.multiple_of(r * 16, 16), 16)
            dst[rows, :] = dst[rows, :] + other[rows, :]
            return carry

        lax.fori_loop(0, tokens // 16, rows16, 0)

    t_copy.wait()
    for n, offset in enumerate((-1, 1)):
        normalize(offset, snd.at[n])
        sent.append(send(snd.at[n], rcv.at[n], d_ss.at[n], d_rs.at[n], {"c": 1 - c}))
    forward(1)
    extra(3)
    extra(1)
    normalize(-2, blk.at[0])
    normalize(2, blk.at[2])
    arrived(rcv.at[1 - c], d_ss.at[1 - c], d_rs.at[1 - c])

    def merge_far(i, carry):
        merge(blk.at[2 * (1 - c), i], rcv.at[1 - c, i])
        return carry

    lax.fori_loop(0, 2 * N, merge_far, 0)
    order = [(q, s) for s in range(N) for q in (1, 0)]
    for q, s in order:
        i = chunk(q, place(s))
        sent.append(
            send(blk.at[2 * zh, i], yrcv.at[i], y_ss.at[i], y_rs.at[i], {"y": y_to})
        )
    normalize(0, blk.at[1])
    arrived(rcv.at[c], d_ss.at[c], d_rs.at[c])

    def merge_near(i, carry):
        merge(blk.at[1, i], rcv.at[c, i])
        return carry

    lax.fori_loop(0, 2 * N, merge_near, 0)
    def near(n):
        q, s = order[n]
        i = chunk(q, place(s))
        dst = tl.at[q * N + zl]
        if (q, s) == (0, N - 1):
            own = pltpu.make_async_copy(blk.at[1, i], dst, loc_sem.at[3])
            own.start()
            own.wait()
        else:
            where = {"x": xp if q else x, "zl": place(s)}
            sent.append(send(blk.at[1, i], dst, l_ss.at[q * N + s], l_rs.at[q * N + zl], where))

    near(0)
    near(1)
    for n, (q, s) in enumerate(order):
        i = chunk(q, place(s))
        slot = q * N + zl
        arrived(yrcv.at[i], y_ss.at[i], y_rs.at[i])
        merge(blk.at[2 * (1 - zh), i], yrcv.at[i])
        where = {"zh": 1 - zh, "x": xp if q else x, "zl": place(s)}
        sent.append(
            send(blk.at[2 * (1 - zh), i], tc.at[slot], k_ss.at[q * N + s], k_rs.at[slot], where)
        )
        if n + 2 < 2 * N:
            near(n + 2)
        if n == 1:
            forward(2)
        if n == 3:
            forward(3)
            for j in (2, 0):
                z = place(2 + j // 2)
                arrived(xall.at[N + z], xx_ss.at[z], x_rs.at[N + z])
                extra(j)

    for n, (kx, kz) in enumerate(others):
        d = lax.rem(x + kx, N) * N + z_at(kz)
        arrived(cnt.at[d], c_ss.at[n], c_rs.at[d])
    total = cnt[0, 0:1, 0:1]
    for d in range(1, N * N):
        total = total + cnt[d, 0:1, 0:1]
    total = total.astype(F32)
    factor = loss_scale / total
    x_copy.wait()
    w_copy.wait()
    arrived(wpair.at[1 - half], w_ss, w_rs)
    sq[...] = jnp.zeros_like(sq)

    def token_block(q, z, n):
        slot = q * N + z
        d = jnp.where(q == 1, xp, x) * N + z
        row = lax.broadcasted_iota(jnp.int32, (tokens, width), 0)
        valid = jnp.where(row < cnt[d, 0:1, 0:1], F32(1.0), F32(0.0))
        base = pl.multiple_of(n * tokens, tokens)
        nt = (((1,), (1,)), ((), ()))
        for e in range(2):
            at = slice(e * width, (e + 1) * width)
            target = tl[slot, :, at].astype(F32) + tc[slot, :, at].astype(F32)
            got = lax.dot_general(xall[slot], wpair[e], nt, preferred_element_type=F32)
            residual = got - target
            masked = valid * residual
            sq[...] += jnp.sum(masked * residual, axis=0, keepdims=True)
            sall[e, pl.ds(base, tokens), :] = (masked * factor).astype(BF16)
        for m in range(4):
            cols = slice(m * 512, (m + 1) * 512)
            part = jnp.dot(
                sall[0, pl.ds(base, tokens), :], wpair[0, :, cols], preferred_element_type=F32
            )
            part += jnp.dot(
                sall[1, pl.ds(base, tokens), :], wpair[1, :, cols], preferred_element_type=F32
            )
            grads[slot, :, cols] = part.astype(BF16)

    step = 256

    def outer(e, terms, cols):
        value = None
        for t, mine in terms:
            if mine:
                left_rows = sall[e, 2 * t * tokens : (2 * t + 2) * tokens, :]
                blocks = [xall[N + place(t), :, cols], xall[place(t), :, cols]]
            else:
                left_rows = sex[2 * (t - 2) : 2 * (t - 1)].reshape(2 * tokens, width)
                blocks = [xex[2 * (t - 2), :, cols], xex[2 * (t - 2) + 1, :, cols]]
            part = lax.dot_general(
                left_rows,
                jnp.concatenate(blocks, axis=0),
                (((0,), (0,)), ((), ())),
                preferred_element_type=F32,
            )
            value = part if value is None else value + part
        return value

    def project(write):
        def columns(j, carry):
            write(pl.ds(pl.multiple_of(j * step, step), step))
            return carry

        lax.fori_loop(0, students // step, columns, 0)

    def to_partner(cols):
        psend[:, cols] = outer(1 - half, ((0, True), (1, True)), cols).astype(BF16)

    def first_steps(cols):
        terms = ((0, True), (1, True), (2, True))
        pown[:, cols] = outer(half, terms, cols)

    def last_step(cols):
        value = pown[:, cols] + precv[:, cols].astype(F32)
        value = value + outer(half, ((3, True), (2, False), (3, False)), cols)
        pout[:, cols] = value.astype(BF16)

    def extra_arrived(t):
        for j in (2 * (t - 2), 2 * (t - 2) + 1):
            arrived(xex.at[j], xe_ss.at[j], xe_rs.at[j])
            arrived(sex.at[j], se_ss.at[j], se_rs.at[j])

    def partner_piece(n):
        return sall.at[1 - half, pl.ds(pl.multiple_of(n * tokens, tokens), tokens)]

    def toward(s):
        return jnp.where(place(s) > zl, 0, 1)

    def add_rows(z, more, write):
        def rows16(r, carry):
            rows = pl.ds(pl.multiple_of(r * 16, 16), 16)
            both = grads[z, rows, :].astype(F32) + xrecv[z, rows, :].astype(F32)
            for way in more:
                both = both + acc[way, z, rows, :].astype(F32)
            write(rows, both.astype(BF16))
            return carry

        lax.fori_loop(0, tokens // 16, rows16, 0)

    def along(s, act):
        z, way = place(s), toward(s)
        act(
            zsend.at[s],
            acc.at[way, z],
            gz_ss.at[s],
            gz_rs.at[way * N + z],
            {"zl": zl + 1 - 2 * way},
        )

    def pass_on(s):
        z, way = place(s), toward(s)
        joined = jnp.where(way == 0, zl > 0, zl < N - 1)

        def put(rows, value):
            zsend[s, rows, :] = value

        arrived(xrecv.at[z], gx_ss.at[z], gx_rs.at[z])

        @pl.when(joined)
        def _():
            arrived(acc.at[way, z], gz_ss.at[s], gz_rs.at[way * N + z])
            add_rows(z, (way,), put)

        @pl.when(jnp.logical_not(joined))
        def _():
            add_rows(z, (), put)

        along(s, send)

    def one_block(n, carry):
        s, q = lax.div(n, 2), 1 - lax.rem(n, 2)
        z = place(s)
        slot = q * N + z

        @pl.when(n == 4)
        def _():
            project(to_partner)
            send(psend, precv, p_ss, p_rs, {"x": wp})

        @pl.when(n == 6)
        def _():
            project(first_steps)

        @pl.when(n < 2 * N - 1)
        def _():
            arrived(tl.at[slot], l_ss.at[slot], l_rs.at[slot])

        @pl.when((q == 1) & (s < 2))
        def _():
            arrived(xall.at[slot], xx_ss.at[z], x_rs.at[slot])

        arrived(tc.at[slot], k_ss.at[slot], k_rs.at[slot])
        token_block(q, z, n)

        @pl.when(q == 1)
        def _():
            send(grads.at[slot], xrecv.at[z], gx_ss.at[z], gx_rs.at[z], {"x": xp})

        @pl.when(n >= 4)
        def _():
            send(partner_piece(n), sex.at[n - 4], se_ss.at[n - 4], se_rs.at[n - 4], {"x": wp})

        return carry

    lax.fori_loop(0, 2 * N, one_block, 0)

    lsum[me] = jnp.full(lsum.shape[1:], jnp.sum(sq[...]), F32)
    for n, (kx, kz) in enumerate(others):
        where = {"x": lax.rem(x + kx, N), "zl": z_at(kz)}
        sent.append(send(lsum.at[me], lsum.at[me], q_ss.at[n], q_rs.at[me], where))

    for s in range(3):
        pass_on(s)
    arrived(precv, p_ss, p_rs)
    extra_arrived(2)
    extra_arrived(3)
    project(last_step)

    def put_out(rows, value):
        gout[rows, :] = value

    arrived(xrecv.at[zl], gx_ss.at[zl], gx_rs.at[zl])

    @pl.when(zl > 0)
    def _():
        arrived(acc.at[0, zl], gz_ss.at[0], gz_rs.at[zl])

    @pl.when(zl < N - 1)
    def _():
        arrived(acc.at[1, zl], gz_ss.at[0], gz_rs.at[N + zl])

    for low, high, ways in ((0, 1, (1,)), (1, N - 1, (0, 1)), (N - 1, N, (0,))):

        @pl.when((zl >= low) & (zl < high))
        def _():
            add_rows(zl, ways, put_out)

    for n, (kx, kz) in enumerate(others):
        d = lax.rem(x + kx, N) * N + z_at(kz)
        arrived(lsum.at[d], q_ss.at[n], q_rs.at[d])
    squares = lsum[0]
    for d in range(1, N * N):
        squares = squares + lsum[d]
    loss[0] = jnp.max(squares / (total * rest))

    def drain(src, dst, ss, rs, where):
        pltpu.make_async_remote_copy(
            src_ref=src, dst_ref=dst, send_sem=ss, recv_sem=rs, device_id=where, device_id_type=MESH
        ).wait_send()

    right(zl, drain)
    left(zl, drain)
    across(zl, drain)
    for j in (1, 2, 3):
        from_left(j, drain)
        from_right(j, drain)

    def far_sent(z, carry):
        drain(grads.at[N + z], xrecv.at[z], gx_ss.at[z], gx_rs.at[z], {"x": xp})
        return carry

    lax.fori_loop(0, N, far_sent, 0)
    drain(psend, precv, p_ss, p_rs, {"x": wp})
    for s in range(3):
        along(s, drain)
    for n in range(4, 2 * N):
        drain(partner_piece(n), sex.at[n - 4], se_ss.at[n - 4], se_rs.at[n - 4], {"x": wp})
    for copy in sent:
        copy.wait_send()


DT_GROUPS = 16


def per_device(student_states, teacher_states, projector, layer_map, boundaries, valid_counts):
    slots, tokens, features = teacher_states.shape
    students = student_states.shape[2]
    weights = jnp.swapaxes(projector, 1, 2)
    width = weights.shape[1]
    any_space = pl.BlockSpec(memory_space=pl.ANY)
    smem = pl.BlockSpec(memory_space=pltpu.SMEM)
    vmem = pl.BlockSpec(memory_space=pltpu.VMEM)
    dma = pltpu.SemaphoreType.DMA
    piece = (2 * N, tokens, 2 * width)
    gout, pout, loss = pl.pallas_call(
        kernel,
        out_shape=(
            jax.ShapeDtypeStruct((tokens, students), BF16),
            jax.ShapeDtypeStruct((width, students), BF16),
            jax.ShapeDtypeStruct((1,), F32),
        ),
        in_specs=[smem, smem, smem, any_space, any_space, any_space],
        out_specs=(vmem, vmem, smem),
        scratch_shapes=[
            pltpu.VMEM((slots, tokens, features), BF16),
            pltpu.VMEM((3, *piece), BF16),
            pltpu.VMEM((2, *piece), BF16),
            pltpu.VMEM((2, *piece), BF16),
            pltpu.VMEM(piece, BF16),
            pltpu.VMEM((2 * N, tokens, students), BF16),
            pltpu.VMEM((2, width, students), BF16),
            pltpu.VMEM(piece, BF16),
            pltpu.VMEM(piece, BF16),
            pltpu.VMEM((2, 2 * N * tokens, width), BF16),
            pltpu.VMEM((2 * N, tokens, students), BF16),
            pltpu.VMEM((N, tokens, students), BF16),
            pltpu.VMEM((3, tokens, students), BF16),
            pltpu.VMEM((2, N, tokens, students), BF16),
            pltpu.VMEM((width, students), BF16),
            pltpu.VMEM((width, students), BF16),
            pltpu.VMEM((width, students), F32),
            pltpu.VMEM((4, tokens, students), BF16),
            pltpu.VMEM((4, tokens, width), BF16),
            pltpu.VMEM((N * N, 8, 128), jnp.int32),
            pltpu.VMEM((N * N, 8, 128), F32),
            pltpu.VMEM((1, width), F32),
            dma((4,)),
            dma((N,)),
            dma((N,)),
            dma((N,)),
            dma((2 * N,)),
            dma,
            dma,
            dma((16,)),
            dma((16,)),
            dma((2,)),
            dma((2,)),
            dma((2 * N,)),
            dma((2 * N,)),
            dma((2 * N,)),
            dma((2 * N,)),
            dma((2 * N,)),
            dma((2 * N,)),
            dma((N,)),
            dma((N,)),
            dma((3,)),
            dma((2 * N,)),
            dma,
            dma,
            dma((4,)),
            dma((4,)),
            dma((4,)),
            dma((4,)),
            dma((16,)),
            dma((16,)),
        ],
        compiler_params=pltpu.CompilerParams(
            collective_id=0, has_side_effects=True, vmem_limit_bytes=67043328
        ),
    )(layer_map, boundaries, valid_counts, student_states, teacher_states, weights)
    return gout[None], jnp.swapaxes(pout, 0, 1)[None], loss


def solution(mesh):
    axes = ("y", "zh", "c", "x", "zl")
    split = Mesh(mesh.devices.reshape(4, 2, 2, N, N), axes)
    section, dp = axes[:3], axes[3:]
    return jax.shard_map(
        per_device,
        mesh=split,
        in_specs=(P(section, dp, None), P(section, dp, None), P(section, None, dp), P(), P(), P(dp)),
        out_specs=(P(section, dp, None), P(section, None, dp), P(section)),
        check_vma=False,
    )
```

```python
import functools

import jax
import jax.numpy as jnp
from jax import lax
from jax.experimental import pallas as pl
from jax.experimental.pallas import tpu as pltpu
from jax.sharding import Mesh
from jax.sharding import PartitionSpec as P

F32 = jnp.float32
BF16 = jnp.bfloat16
MESH = pl.DeviceIdType.MESH
loss_scale = 128.0
norm_eps = 1e-06
N = 4


def kernel(
    lm,
    bd,
    vc,
    x_hbm,
    t_hbm,
    w_hbm,
    gout,
    pout,
    loss,
    tv,
    blk,
    snd,
    rcv,
    yrcv,
    xall,
    wpair,
    tl,
    tc,
    sall,
    grads,
    xrecv,
    zsend,
    acc,
    psend,
    precv,
    pown,
    xex,
    sex,
    cnt,
    lsum,
    sq,
    loc_sem,
    xr_ss,
    xl_ss,
    xx_ss,
    x_rs,
    w_ss,
    w_rs,
    c_ss,
    c_rs,
    d_ss,
    d_rs,
    y_ss,
    y_rs,
    l_ss,
    l_rs,
    k_ss,
    k_rs,
    gx_ss,
    gx_rs,
    gz_ss,
    gz_rs,
    p_ss,
    p_rs,
    xe_ss,
    xe_rs,
    se_ss,
    se_rs,
    q_ss,
    q_rs,
):
    y, zh, c = lax.axis_index("y"), lax.axis_index("zh"), lax.axis_index("c")
    x, zl = lax.axis_index("x"), lax.axis_index("zl")
    here = y * 4 + zh * 2 + c
    me = x * N + zl
    xp = 3 - x
    half, pair = lax.rem(x, 2), lax.div(x, 2)
    wp = x + 1 - 2 * half
    y_to = lax.rem(y + 2 * zh - 1 + 4, 4)
    y_from = lax.rem(y - 2 * zh + 1 + 4, 4)
    tokens = x_hbm.shape[1]
    width = w_hbm.shape[1]
    students = w_hbm.shape[2]
    rest = DT_GROUPS * width

    def z_at(k):
        return lax.rem(zl + k, N)

    def goal(s):
        return lax.rem(zl + s + 1, N)

    def source(s):
        return lax.rem(zl + 3 - s, N)

    upper = zl >= N // 2
    inward = jnp.where(upper, N - 1 - zl, zl)

    def place(s):
        z = jnp.where(s == 0, 3, jnp.where(s == 1, 2, jnp.where(s == 2, 1 - inward, inward)))
        return jnp.where(upper, N - 1 - z, z)

    def send(src, dst, ss, rs, where):
        copy = pltpu.make_async_remote_copy(
            src_ref=src, dst_ref=dst, send_sem=ss, recv_sem=rs, device_id=where, device_id_type=MESH
        )
        copy.start()
        return copy

    def arrived(dst, ss, rs):
        pltpu.make_async_remote_copy(
            src_ref=dst,
            dst_ref=dst,
            send_sem=ss,
            recv_sem=rs,
            device_id={"c": 1 - c},
            device_id_type=MESH,
        ).wait_recv()

    sent = []
    t_copy = pltpu.make_async_copy(t_hbm, tv, loc_sem.at[0])
    t_copy.start()
    x_copy = pltpu.make_async_copy(x_hbm.at[0], xall.at[zl], loc_sem.at[1])
    x_copy.start()
    w_copy = pltpu.make_async_copy(w_hbm.at[0], wpair.at[half], loc_sem.at[2])
    w_copy.start()
    cnt[me] = jnp.full(cnt.shape[1:], vc[0], jnp.int32)

    others = [(kx, kz) for kx in range(N) for kz in range(N) if (kx, kz) != (0, 0)]
    barrier = pltpu.get_barrier_semaphore()
    greeted = [{"c": 1 - c}, {"y": y_to}, {"y": y_from}]
    greeted += [{"x": lax.rem(x + kx, N), "zl": z_at(kz)} for kx, kz in others]
    greeted += [{"zh": 1 - zh, "x": px, "zl": z_at(kz)} for px in (x, xp) for kz in range(N)]
    for where in greeted:
        pl.semaphore_signal(barrier, inc=1, device_id=where, device_id_type=MESH)
    pl.semaphore_wait(barrier, len(greeted))

    def right(b, act):
        @pl.when(zl < N - 1)
        def _():
            act(x_block(b), xall.at[b], xr_ss.at[b], x_rs.at[b], {"zl": zl + 1})

    def left(b, act):
        @pl.when(zl > 0)
        def _():
            act(x_block(b), xall.at[b], xl_ss.at[b], x_rs.at[b], {"zl": zl - 1})

    def across(b, act):
        act(x_block(b), xall.at[N + b], xx_ss.at[b], x_rs.at[N + b], {"x": xp})

    def x_block(b):
        return x_hbm.at[0] if b is zl else xall.at[b]

    def from_left(j, act):
        @pl.when(zl - j >= 0)
        def _():
            right(zl - j, act)
            across(zl - j, act)

    def from_right(j, act):
        @pl.when(zl + j < N)
        def _():
            left(zl + j, act)
            across(zl + j, act)

    def forward(j):
        @pl.when(zl - j >= 0)
        def _():
            arrived(xall.at[zl - j], xx_ss.at[zl - j], x_rs.at[zl - j])

        from_left(j, send)

        @pl.when(zl + j < N)
        def _():
            arrived(xall.at[zl + j], xx_ss.at[zl + j], x_rs.at[zl + j])

        from_right(j, send)

    def extra(j, act):
        slot = (1 - j % 2) * N + source(2 + j // 2)
        block = x_hbm.at[0] if j == 3 else xall.at[slot]
        act(block, xex.at[j], xe_ss.at[j], xe_rs.at[j], {"x": wp})

    right(zl, send)
    left(zl, send)
    across(zl, send)
    sent.append(send(w_hbm.at[0], wpair.at[half], w_ss, w_rs, {"x": wp}))
    for n, (kx, kz) in enumerate(others):
        where = {"x": lax.rem(x + kx, N), "zl": z_at(kz)}
        sent.append(send(cnt.at[me], cnt.at[me], c_ss.at[n], c_rs.at[me], where))

    def plan(offset):
        to = here + offset
        inside = (to >= 0) & (to < 16)
        layer = lm[jnp.clip(to, 0, 15)]
        owner = jnp.int32(0)
        for k in range(1, 16):
            owner = owner + jnp.where(bd[k] <= layer, 1, 0)
        slot = jnp.clip(layer - bd[here], 0, tv.shape[0] - 1)
        return slot, jnp.where(inside & (owner == here), F32(1.0), F32(0.0))

    def normalize(offset, dst):
        slot, keep = plan(offset)

        def rows16(r, carry):
            rows = pl.ds(pl.multiple_of(r * 16, 16), 16)
            h = tv[slot, rows, :].astype(F32)
            scale = lax.rsqrt(jnp.mean(h * h, axis=1, keepdims=True) + norm_eps) * keep
            out = (h * scale).astype(BF16)
            for p in range(2):
                for z in range(N):
                    for e in range(2):
                        at = width * (8 * p + 4 * e + z)
                        dst[p * N + z, rows, e * width : (e + 1) * width] = out[:, at : at + width]
            return carry

        lax.fori_loop(0, tokens // 16, rows16, 0)

    def chunk(q, z):
        return (pair + q - 2 * pair * q) * N + z

    def merge(dst, other):
        def rows16(r, carry):
            rows = pl.ds(pl.multiple_of(r * 16, 16), 16)
            dst[rows, :] = dst[rows, :] + other[rows, :]
            return carry

        lax.fori_loop(0, tokens // 16, rows16, 0)

    t_copy.wait()
    for n, offset in enumerate((-1, 1)):
        normalize(offset, snd.at[n])
        sent.append(send(snd.at[n], rcv.at[n], d_ss.at[n], d_rs.at[n], {"c": 1 - c}))
    forward(1)
    extra(3, send)
    normalize(-2, blk.at[0])
    normalize(2, blk.at[2])
    arrived(rcv.at[1 - c], d_ss.at[1 - c], d_rs.at[1 - c])

    def merge_far(i, carry):
        merge(blk.at[2 * (1 - c), i], rcv.at[1 - c, i])
        return carry

    lax.fori_loop(0, 2 * N, merge_far, 0)
    order = [(q, s) for s in range(N) for q in (1, 0)]
    for q, s in order:
        i = chunk(q, goal(s))
        sent.append(
            send(blk.at[2 * zh, i], yrcv.at[i], y_ss.at[i], y_rs.at[i], {"y": y_to})
        )
    normalize(0, blk.at[1])
    arrived(rcv.at[c], d_ss.at[c], d_rs.at[c])

    def merge_near(i, carry):
        merge(blk.at[1, i], rcv.at[c, i])
        return carry

    lax.fori_loop(0, 2 * N, merge_near, 0)
    def near(n):
        q, s = order[n]
        i = chunk(q, goal(s))
        dst = tl.at[q * N + zl]
        if (q, s) == (0, N - 1):
            own = pltpu.make_async_copy(blk.at[1, i], dst, loc_sem.at[3])
            own.start()
            own.wait()
        else:
            where = {"x": xp if q else x, "zl": goal(s)}
            sent.append(send(blk.at[1, i], dst, l_ss.at[q * N + s], l_rs.at[q * N + zl], where))

    near(0)
    near(1)
    for n, (q, s) in enumerate(order):
        i = chunk(q, goal(s))
        slot = q * N + zl
        arrived(yrcv.at[i], y_ss.at[i], y_rs.at[i])
        merge(blk.at[2 * (1 - zh), i], yrcv.at[i])
        where = {"zh": 1 - zh, "x": xp if q else x, "zl": goal(s)}
        sent.append(
            send(blk.at[2 * (1 - zh), i], tc.at[slot], k_ss.at[q * N + s], k_rs.at[slot], where)
        )
        if n + 2 < 2 * N:
            near(n + 2)
        if n == 1:
            forward(2)
        if n == 3:
            forward(3)
            extra(1, send)
            arrived(xall.at[N + zl], xx_ss.at[zl], x_rs.at[N + zl])
            extra(2, send)

    for n, (kx, kz) in enumerate(others):
        d = lax.rem(x + kx, N) * N + z_at(kz)
        arrived(cnt.at[d], c_ss.at[n], c_rs.at[d])
    total = cnt[0, 0:1, 0:1]
    for d in range(1, N * N):
        total = total + cnt[d, 0:1, 0:1]
    total = total.astype(F32)
    factor = loss_scale / total
    x_copy.wait()
    w_copy.wait()
    arrived(wpair.at[1 - half], w_ss, w_rs)
    sq[...] = jnp.zeros_like(sq)

    def token_block(q, z, n):
        slot = q * N + z
        d = jnp.where(q == 1, xp, x) * N + z
        row = lax.broadcasted_iota(jnp.int32, (tokens, width), 0)
        valid = jnp.where(row < cnt[d, 0:1, 0:1], F32(1.0), F32(0.0))
        base = pl.multiple_of(n * tokens, tokens)
        nt = (((1,), (1,)), ((), ()))
        for e in range(2):
            at = slice(e * width, (e + 1) * width)
            target = tl[slot, :, at].astype(F32) + tc[slot, :, at].astype(F32)
            got = lax.dot_general(xall[slot], wpair[e], nt, preferred_element_type=F32)
            residual = got - target
            masked = valid * residual
            sq[...] += jnp.sum(masked * residual, axis=0, keepdims=True)
            sall[e, pl.ds(base, tokens), :] = (masked * factor).astype(BF16)
        for m in range(4):
            cols = slice(m * 512, (m + 1) * 512)
            part = jnp.dot(
                sall[0, pl.ds(base, tokens), :], wpair[0, :, cols], preferred_element_type=F32
            )
            part += jnp.dot(
                sall[1, pl.ds(base, tokens), :], wpair[1, :, cols], preferred_element_type=F32
            )
            grads[slot, :, cols] = part.astype(BF16)

    step = 256

    def outer(e, terms, cols):
        value = None
        for t, mine in terms:
            if mine:
                left_rows = sall[e, 2 * t * tokens : (2 * t + 2) * tokens, :]
                blocks = [xall[N + source(t), :, cols], xall[source(t), :, cols]]
            else:
                left_rows = sex[2 * (t - 2) : 2 * (t - 1)].reshape(2 * tokens, width)
                blocks = [xex[2 * (t - 2), :, cols], xex[2 * (t - 2) + 1, :, cols]]
            part = lax.dot_general(
                left_rows,
                jnp.concatenate(blocks, axis=0),
                (((0,), (0,)), ((), ())),
                preferred_element_type=F32,
            )
            value = part if value is None else value + part
        return value

    def project(write):
        def columns(j, carry):
            write(pl.ds(pl.multiple_of(j * step, step), step))
            return carry

        lax.fori_loop(0, students // step, columns, 0)

    def to_partner(cols):
        psend[:, cols] = outer(1 - half, ((0, True), (1, True)), cols).astype(BF16)

    def first_steps(cols):
        terms = ((0, True), (1, True), (2, True))
        pown[:, cols] = outer(half, terms, cols)

    def last_step(cols):
        value = pown[:, cols] + precv[:, cols].astype(F32)
        value = value + outer(half, ((3, True), (2, False), (3, False)), cols)
        pout[:, cols] = value.astype(BF16)

    def extra_arrived(t):
        for j in (2 * (t - 2), 2 * (t - 2) + 1):
            arrived(xex.at[j], xe_ss.at[j], xe_rs.at[j])
            arrived(sex.at[j], se_ss.at[j], se_rs.at[j])

    def partner_piece(n):
        return sall.at[1 - half, pl.ds(pl.multiple_of(n * tokens, tokens), tokens)]

    def toward(s):
        return jnp.where(place(s) > zl, 0, 1)

    def add_rows(z, more, write):
        def rows16(r, carry):
            rows = pl.ds(pl.multiple_of(r * 16, 16), 16)
            both = grads[z, rows, :].astype(F32) + xrecv[z, rows, :].astype(F32)
            for way in more:
                both = both + acc[way, z, rows, :].astype(F32)
            write(rows, both.astype(BF16))
            return carry

        lax.fori_loop(0, tokens // 16, rows16, 0)

    def along(s, act):
        z, way = place(s), toward(s)
        act(
            zsend.at[s],
            acc.at[way, z],
            gz_ss.at[s],
            gz_rs.at[way * N + z],
            {"zl": zl + 1 - 2 * way},
        )

    def pass_on(s):
        z, way = place(s), toward(s)
        joined = jnp.where(way == 0, zl > 0, zl < N - 1)

        def put(rows, value):
            zsend[s, rows, :] = value

        arrived(xrecv.at[z], gx_ss.at[z], gx_rs.at[z])

        @pl.when(joined)
        def _():
            arrived(acc.at[way, z], gz_ss.at[s], gz_rs.at[way * N + z])
            add_rows(z, (way,), put)

        @pl.when(jnp.logical_not(joined))
        def _():
            add_rows(z, (), put)

        along(s, send)

    def one_block(n, carry):
        s, q = lax.div(n, 2), 1 - lax.rem(n, 2)
        z = source(s)
        slot = q * N + z

        @pl.when(n == 4)
        def _():
            arrived(xall.at[slot], xx_ss.at[z], x_rs.at[slot])
            extra(0, send)
            project(to_partner)
            send(psend, precv, p_ss, p_rs, {"x": wp})

        @pl.when(n == 6)
        def _():
            project(first_steps)

        @pl.when(n < 2 * N - 1)
        def _():
            arrived(tl.at[slot], l_ss.at[slot], l_rs.at[slot])

        @pl.when((q == 1) & (s < 2))
        def _():
            arrived(xall.at[slot], xx_ss.at[z], x_rs.at[slot])

        arrived(tc.at[slot], k_ss.at[slot], k_rs.at[slot])
        token_block(q, z, n)

        @pl.when(q == 1)
        def _():
            send(grads.at[slot], xrecv.at[z], gx_ss.at[z], gx_rs.at[z], {"x": xp})

        @pl.when(n >= 4)
        def _():
            send(partner_piece(n), sex.at[n - 4], se_ss.at[n - 4], se_rs.at[n - 4], {"x": wp})

        return carry

    lax.fori_loop(0, 2 * N, one_block, 0)

    lsum[me] = jnp.full(lsum.shape[1:], jnp.sum(sq[...]), F32)
    for n, (kx, kz) in enumerate(others):
        where = {"x": lax.rem(x + kx, N), "zl": z_at(kz)}
        sent.append(send(lsum.at[me], lsum.at[me], q_ss.at[n], q_rs.at[me], where))

    for s in range(3):
        pass_on(s)
    arrived(precv, p_ss, p_rs)
    extra_arrived(2)
    extra_arrived(3)
    project(last_step)

    def put_out(rows, value):
        gout[rows, :] = value

    arrived(xrecv.at[zl], gx_ss.at[zl], gx_rs.at[zl])

    @pl.when(zl > 0)
    def _():
        arrived(acc.at[0, zl], gz_ss.at[0], gz_rs.at[zl])

    @pl.when(zl < N - 1)
    def _():
        arrived(acc.at[1, zl], gz_ss.at[0], gz_rs.at[N + zl])

    for low, high, ways in ((0, 1, (1,)), (1, N - 1, (0, 1)), (N - 1, N, (0,))):

        @pl.when((zl >= low) & (zl < high))
        def _():
            add_rows(zl, ways, put_out)

    for n, (kx, kz) in enumerate(others):
        d = lax.rem(x + kx, N) * N + z_at(kz)
        arrived(lsum.at[d], q_ss.at[n], q_rs.at[d])
    squares = lsum[0]
    for d in range(1, N * N):
        squares = squares + lsum[d]
    loss[0] = jnp.max(squares / (total * rest))

    def drain(src, dst, ss, rs, where):
        pltpu.make_async_remote_copy(
            src_ref=src, dst_ref=dst, send_sem=ss, recv_sem=rs, device_id=where, device_id_type=MESH
        ).wait_send()

    right(zl, drain)
    left(zl, drain)
    across(zl, drain)
    for j in (1, 2, 3):
        from_left(j, drain)
        from_right(j, drain)

    def far_sent(z, carry):
        drain(grads.at[N + z], xrecv.at[z], gx_ss.at[z], gx_rs.at[z], {"x": xp})
        return carry

    lax.fori_loop(0, N, far_sent, 0)
    drain(psend, precv, p_ss, p_rs, {"x": wp})
    for s in range(3):
        along(s, drain)
    for j in range(4):
        extra(j, drain)
    for n in range(4, 2 * N):
        drain(partner_piece(n), sex.at[n - 4], se_ss.at[n - 4], se_rs.at[n - 4], {"x": wp})
    for copy in sent:
        copy.wait_send()


DT_GROUPS = 16


def per_device(student_states, teacher_states, projector, layer_map, boundaries, valid_counts):
    slots, tokens, features = teacher_states.shape
    students = student_states.shape[2]
    weights = jnp.swapaxes(projector, 1, 2)
    width = weights.shape[1]
    any_space = pl.BlockSpec(memory_space=pl.ANY)
    smem = pl.BlockSpec(memory_space=pltpu.SMEM)
    vmem = pl.BlockSpec(memory_space=pltpu.VMEM)
    dma = pltpu.SemaphoreType.DMA
    piece = (2 * N, tokens, 2 * width)
    gout, pout, loss = pl.pallas_call(
        kernel,
        out_shape=(
            jax.ShapeDtypeStruct((tokens, students), BF16),
            jax.ShapeDtypeStruct((width, students), BF16),
            jax.ShapeDtypeStruct((1,), F32),
        ),
        in_specs=[smem, smem, smem, any_space, any_space, any_space],
        out_specs=(vmem, vmem, smem),
        scratch_shapes=[
            pltpu.VMEM((slots, tokens, features), BF16),
            pltpu.VMEM((3, *piece), BF16),
            pltpu.VMEM((2, *piece), BF16),
            pltpu.VMEM((2, *piece), BF16),
            pltpu.VMEM(piece, BF16),
            pltpu.VMEM((2 * N, tokens, students), BF16),
            pltpu.VMEM((2, width, students), BF16),
            pltpu.VMEM(piece, BF16),
            pltpu.VMEM(piece, BF16),
            pltpu.VMEM((2, 2 * N * tokens, width), BF16),
            pltpu.VMEM((2 * N, tokens, students), BF16),
            pltpu.VMEM((N, tokens, students), BF16),
            pltpu.VMEM((3, tokens, students), BF16),
            pltpu.VMEM((2, N, tokens, students), BF16),
            pltpu.VMEM((width, students), BF16),
            pltpu.VMEM((width, students), BF16),
            pltpu.VMEM((width, students), F32),
            pltpu.VMEM((4, tokens, students), BF16),
            pltpu.VMEM((4, tokens, width), BF16),
            pltpu.VMEM((N * N, 8, 128), jnp.int32),
            pltpu.VMEM((N * N, 8, 128), F32),
            pltpu.VMEM((1, width), F32),
            dma((4,)),
            dma((N,)),
            dma((N,)),
            dma((N,)),
            dma((2 * N,)),
            dma,
            dma,
            dma((16,)),
            dma((16,)),
            dma((2,)),
            dma((2,)),
            dma((2 * N,)),
            dma((2 * N,)),
            dma((2 * N,)),
            dma((2 * N,)),
            dma((2 * N,)),
            dma((2 * N,)),
            dma((N,)),
            dma((N,)),
            dma((3,)),
            dma((2 * N,)),
            dma,
            dma,
            dma((4,)),
            dma((4,)),
            dma((4,)),
            dma((4,)),
            dma((16,)),
            dma((16,)),
        ],
        compiler_params=pltpu.CompilerParams(
            collective_id=0, has_side_effects=True, vmem_limit_bytes=67043328
        ),
    )(layer_map, boundaries, valid_counts, student_states, teacher_states, weights)
    return gout[None], jnp.swapaxes(pout, 0, 1)[None], loss


def solution(mesh):
    axes = ("y", "zh", "c", "x", "zl")
    split = Mesh(mesh.devices.reshape(4, 2, 2, N, N), axes)
    section, dp = axes[:3], axes[3:]
    return jax.shard_map(
        per_device,
        mesh=split,
        in_specs=(P(section, dp, None), P(section, dp, None), P(section, None, dp), P(), P(), P(dp)),
        out_specs=(P(section, dp, None), P(section, None, dp), P(section)),
        check_vma=False,
    )
```
